16 devices in a mesh: dp: 4 (over z, y), tp: 4 (over x, core).
Axes of the slice: x: 2, y: 2, z: 2, core: 2. Of those that a mesh axis runs over, the one named last changes fastest.
Arguments:
- x: bfloat16 [512, 2048], P('dp'), parts along dimension 0
- g_attn: bfloat16 [2, 2048], replicated
- w_qkv: bfloat16 [2, 2048, 3072], P(None, None, 'tp')
- w_o: bfloat16 [2, 2048, 2048], P(None, 'tp')
- g_mlp: bfloat16 [2, 2048], replicated
- w_gate: bfloat16 [2, 2048, 8192], P(None, None, 'tp')
- w_up: bfloat16 [2, 2048, 8192], P(None, None, 'tp')
- w_down: bfloat16 [2, 8192, 2048], P(None, 'tp')
- k_cache: bfloat16 [2, 512, 512, 8, 64], P(None, 'dp', None, 'tp'), parts along dimension 1
- v_cache: bfloat16 [2, 512, 512, 8, 64], P(None, 'dp', None, 'tp'), parts along dimension 1
- lengths: int32 [512], P('dp'), parts along dimension 0
Outputs:
- output: bfloat16 [512, 2048], P('dp'), parts along dimension 0
There are 4 independent parts. The reference program is written for one: setup_inputs(seed, part) draws one part's arguments, and reference() takes and returns one part's arrays. A program takes and returns all parts, laid end to end along the dimension named above; an argument that names none is the same for every part.
All inputs are finite; a program needn't handle non-finite values.
Results may differ from the reference program's by a relative error of at most 0.018017.
Values are sent between devices in bfloat16 or wider.
A program may use at most 1 GiB of HBM per device.

```python
import jax
import jax.numpy as jnp
from jax import lax

D = 2048
HEADS = 32
KV_HEADS = 8
HEAD = 64
FF = 8192
BATCH = 128
SEQ = 512
LAYERS = 2
TP = 4

GROUP = HEADS // KV_HEADS
QKV = (HEADS + 2 * KV_HEADS) * HEAD
EPS = 1e-5
ROPE_THETA = 500000.0


def setup_inputs(seed: int = 0, part: int = 0) -> dict:
    key = jax.random.PRNGKey(seed)
    ks = jax.random.split(key, 8)
    kp = jax.random.split(jax.random.fold_in(ks[7], part), 5)

    def normal(k, shape, scale):
        return (scale * jax.random.normal(k, shape, jnp.float32)).astype(jnp.bfloat16)

    def gain(k):
        return jax.random.uniform(k, (LAYERS, D), jnp.float32, 0.7, 1.3).astype(jnp.bfloat16)

    g_attn = gain(ks[0])
    w_qkv = normal(ks[1], (LAYERS, D, QKV), D ** -0.5)
    w_o = normal(ks[2], (LAYERS, HEADS * HEAD, D), (HEADS * HEAD) ** -0.5)
    g_mlp = gain(ks[3])
    w_gate = normal(ks[4], (LAYERS, D, FF), D ** -0.5)
    w_up = normal(ks[5], (LAYERS, D, FF), D ** -0.5)
    w_down = normal(ks[6], (LAYERS, FF, D), FF ** -0.5)
    x = normal(kp[0], (BATCH, D), 1.0)
    lengths = jax.random.randint(kp[1], (BATCH,), 1, SEQ, dtype=jnp.int32)
    shape = (LAYERS, BATCH, SEQ, KV_HEADS, HEAD)
    stale = jnp.arange(SEQ)[None, None, :, None, None] >= lengths[None, :, None, None, None]
    k_cache = (2.0 * jax.random.normal(kp[2], shape, jnp.float32)).astype(jnp.bfloat16)
    mu = jax.random.normal(kp[3], (LAYERS, BATCH, 1, KV_HEADS, HEAD), jnp.float32)
    v_cache = 0.7 * mu + jax.random.normal(kp[4], shape, jnp.float32)
    v_cache = jnp.where(stale, v_cache + 2.0, v_cache).astype(jnp.bfloat16)
    return {'x': x, 'g_attn': g_attn, 'w_qkv': w_qkv, 'w_o': w_o, 'g_mlp': g_mlp,
            'w_gate': w_gate, 'w_up': w_up, 'w_down': w_down,
            'k_cache': k_cache, 'v_cache': v_cache, 'lengths': lengths}


def _rmsnorm(x, g):
    xf = x.astype(jnp.float32)
    r = lax.rsqrt(jnp.mean(xf * xf, axis=-1, keepdims=True) + EPS)
    return (xf * r * g.astype(jnp.float32)).astype(jnp.bfloat16)


def _rope(t, pos):
    half = HEAD // 2
    inv = ROPE_THETA ** (-jnp.arange(half, dtype=jnp.float32) * 2.0 / HEAD)
    ang = pos.astype(jnp.float32)[:, None] * inv[None, :]
    shape = (pos.shape[0],) + (1,) * (t.ndim - 2) + (half,)
    c = jnp.cos(ang).reshape(shape)
    s = jnp.sin(ang).reshape(shape)
    tf = t.astype(jnp.float32)
    t1, t2 = tf[..., :half], tf[..., half:]
    return jnp.concatenate([t1 * c - t2 * s, t2 * c + t1 * s], axis=-1).astype(jnp.bfloat16)


def _attend(q, k_new, v_new, kc, vc, length):
    scale = HEAD ** -0.5
    qf = q.astype(jnp.float32)
    s_c = jnp.einsum('jgd,sjd->jgs', qf, kc.astype(jnp.float32)) * scale
    s_c = jnp.where(jnp.arange(SEQ)[None, None, :] < length, s_c, -jnp.inf)
    s_n = jnp.einsum('jgd,jd->jg', qf, k_new.astype(jnp.float32)) * scale
    m = jnp.maximum(jnp.max(s_c, axis=-1), s_n)
    p_c = jnp.exp(s_c - m[..., None])
    p_n = jnp.exp(s_n - m)
    den = jnp.sum(p_c, axis=-1) + p_n
    o = jnp.einsum('jgs,sjd->jgd', p_c.astype(jnp.bfloat16).astype(jnp.float32), vc.astype(jnp.float32))
    o = o + p_n[..., None] * v_new.astype(jnp.float32)[:, None, :]
    return o / den[..., None]


def _row_parallel(a, w):
    n = w.shape[0] // TP
    return sum(jnp.dot(a[:, i * n:(i + 1) * n], w[i * n:(i + 1) * n], preferred_element_type=jnp.float32)
               .astype(jnp.bfloat16).astype(jnp.float32) for i in range(TP))


def _layer(x, lengths, g1, wqkv, wo, g2, wg, wu, wd, kc, vc):
    a = _rmsnorm(x, g1)
    qkv = jnp.dot(a, wqkv, preferred_element_type=jnp.float32).astype(jnp.bfloat16)
    qkv = qkv.reshape(BATCH, KV_HEADS, GROUP + 2, HEAD)
    q = _rope(qkv[:, :, :GROUP], lengths)
    k = _rope(qkv[:, :, GROUP], lengths)
    v = qkv[:, :, GROUP + 1]
    att = lax.map(lambda t: _attend(*t), (q, k, v, kc, vc, lengths))
    att = att.astype(jnp.bfloat16).reshape(BATCH, HEADS * HEAD)
    h = (x.astype(jnp.float32) + _row_parallel(att, wo)).astype(jnp.bfloat16)
    b = _rmsnorm(h, g2)
    gate = jnp.dot(b, wg, preferred_element_type=jnp.float32)
    up = jnp.dot(b, wu, preferred_element_type=jnp.float32)
    act = (jax.nn.silu(gate) * up).astype(jnp.bfloat16)
    return (h.astype(jnp.float32) + _row_parallel(act, wd)).astype(jnp.bfloat16)


def reference(x, g_attn, w_qkv, w_o, g_mlp, w_gate, w_up, w_down, k_cache, v_cache, lengths):
    def body(h, p):
        return _layer(h, lengths, *p), None
    y, _ = lax.scan(body, x, (g_attn, w_qkv, w_o, g_mlp, w_gate, w_up, w_down, k_cache, v_cache))
    return y
```

```python
import functools

import jax
import jax.numpy as jnp
import numpy as np
from jax import lax
from jax.experimental import pallas as pl
from jax.experimental.pallas import tpu as pltpu
from jax.sharding import PartitionSpec as P

EPS = 1e-5
ROPE_THETA = 500000.0
MESH = pl.DeviceIdType.MESH
F32, BF16 = jnp.float32, jnp.bfloat16

LAYERS, ROWS, D, SEQ, HD = 2, 128, 2048, 512, 64
QKVL, FFL, HEADS = 768, 2048, 8
CB, NCB = 256, 8
CHUNK, NCH = 8, 16
RING = 12
LEAD = (6, RING)
QR, NQ = 32, 4
SCALE = HD ** -0.5
NT = (((1,), (1,)), ((), ()))


def _dot(a, b):
    return jnp.dot(a, b, preferred_element_type=F32)


def _kernel(lens, lenv, inv, g_attn, g_mlp, x_hbm, wqkv_hbm, wo_hbm, wg_hbm, wu_hbm, wd_hbm, k_hbm, v_hbm,
            out_hbm,
            kbuf, vbuf, wqkv, wo, wg, wu, wd, xb, hb, an, act, to, tm, r1o, r1m, co, cm, r2o, r2m,
            qkvs, qs, os_, kn, vn, cs, sn, pbuf, stat,
            ksem, vsem, qsem, osem, gsem, usem, dsem, xsem, ysem,
            s1o, a1o, s2o, a2o, s3o, a3o, s1m, a1m, s2m, a2m, s3m, a3m):
    me = lax.axis_index("tp")
    core = lax.rem(me, 2)
    partner = me + 1 - 2 * core
    across = lax.rem(me + 2, 4)
    barrier = pltpu.get_barrier_semaphore()
    for dev in (partner, across):
        pl.semaphore_signal(barrier, inc=1, device_id={"tp": dev}, device_id_type=MESH)

    def slot_of(l, c):
        return lax.rem(l * NCH + c, RING)

    def kcopy(l, c):
        s = slot_of(l, c)
        return pltpu.make_async_copy(k_hbm.at[l, pl.ds(c * CHUNK, CHUNK)], kbuf.at[s], ksem.at[s])

    def vcopy(l, c):
        s = slot_of(l, c)
        return pltpu.make_async_copy(v_hbm.at[l, pl.ds(c * CHUNK, CHUNK)], vbuf.at[s], vsem.at[s])

    def qcopy(l, i):
        r = pl.ds(i * 512, 512)
        return pltpu.make_async_copy(wqkv_hbm.at[l, r], wqkv.at[r], qsem.at[i])

    def ocopy(l, i):
        r = pl.ds(i * 256, 256)
        return pltpu.make_async_copy(wo_hbm.at[l, r], wo.at[r], osem.at[i])

    def gcopy(l, i):
        return pltpu.make_async_copy(wg_hbm.at[l, :, pl.ds(i * 512, 512)], wg.at[i], gsem.at[i])

    def ucopy(l, i):
        return pltpu.make_async_copy(wu_hbm.at[l, :, pl.ds(i * 512, 512)], wu.at[i], usem.at[i])

    def dcopy(l, i):
        return pltpu.make_async_copy(wd_hbm.at[l, :, pl.ds(i * CB, CB)], wd.at[i], dsem.at[i])

    def xcopy(i):
        return pltpu.make_async_copy(x_hbm.at[:, pl.ds(i * CB, CB)], xb.at[i], xsem.at[i])

    def ycopy(i):
        return pltpu.make_async_copy(xb.at[i], out_hbm.at[:, pl.ds(i * CB, CB)], ysem.at[i])

    def remote(src, dst, send, recv, dev):
        return pltpu.make_async_remote_copy(src_ref=src, dst_ref=dst, send_sem=send, recv_sem=recv,
                                            device_id={"tp": dev}, device_id_type=MESH)

    for i in range(NCB):
        xcopy(i).start()
    for i in range(4):
        qcopy(0, i).start()
    for c in range(LEAD[0]):
        kcopy(0, c).start()
        vcopy(0, c).start()
        if c == 1:
            for i in range(2):
                ocopy(0, i).start()

    lane = lax.broadcasted_iota(jnp.int32, (ROWS, 128), 1)
    low = lane < 64
    first = lax.rem(lane, 64) < 32

    pos = jnp.transpose(jnp.broadcast_to(lenv[...].astype(F32), (ROWS, 128)))
    ang = pos * inv[...]
    cs[...] = jnp.cos(ang)
    sn[...] = jnp.where(first, -jnp.sin(ang), jnp.sin(ang))

    def norm_rows(src, r0, g_ref, l):
        rows = pl.ds(r0, QR)
        ss = jnp.zeros((QR, CB), F32)
        for kb in range(NCB):
            v = src[kb, rows, :].astype(F32)
            ss = ss + v * v
        r = lax.rsqrt(jnp.sum(ss, axis=-1, keepdims=True) * (1.0 / D) + EPS)
        for kb in range(NCB):
            v = src[kb, rows, :].astype(F32)
            g = g_ref[l:l + 1, kb * CB:(kb + 1) * CB].astype(F32)
            an[rows, kb * CB:(kb + 1) * CB] = (v * r * g).astype(BF16)

    def rope(t):
        other = jnp.where(first, pltpu.roll(t, 96, 1), pltpu.roll(t, 32, 1))
        return (t * cs[...] + other * sn[...]).astype(BF16).astype(F32)

    def project(l):
        for i in range(4):
            qcopy(l, i).wait()
        for nb in range(3):
            z = _dot(an[...], wqkv[:, nb * 256:(nb + 1) * 256]).astype(BF16).astype(F32)
            qkvs[2 * nb] = z[:, :128]
            qkvs[2 * nb + 1] = z[:, 128:]
        for j in range(2):
            for pr in range(2):
                t = rope(qkvs[3 * j + pr])
                swapped = pltpu.roll(t, 64, 1)
                h = 4 * j + 2 * pr
                if j == 0:
                    even, odd = jnp.where(low, t, 0.0), jnp.where(low, swapped, 0.0)
                else:
                    even, odd = jnp.where(low, 0.0, swapped), jnp.where(low, 0.0, t)
                qs[pl.ds(h, ROWS, stride=HEADS), :] = even
                qs[pl.ds(h + 1, ROWS, stride=HEADS), :] = odd
        k0, k1 = rope(qkvs[2]), rope(qkvs[5])
        kn[...] = jnp.where(low, k0, pltpu.roll(k1, 64, 1))
        vn[...] = jnp.where(low, pltpu.roll(qkvs[2], 64, 1), qkvs[5])

    pos_s = lax.broadcasted_iota(jnp.int32, (8, SEQ), 1)

    def scores(l, c):
        s_ = slot_of(l, c)
        par = lax.rem(c, 2)
        for t in range(CHUNK):
            b = c * CHUNK + t
            q = qs[pl.ds(b * 8, 8), :]
            new = jnp.sum(q * kn[pl.ds(b, 1), :], axis=-1, keepdims=True) * SCALE
            s = _dot(q.astype(BF16), kbuf[s_, t]) * SCALE
            s = jnp.where(pos_s < lens[b], s, -jnp.inf)
            m = jnp.maximum(jnp.max(s, axis=-1, keepdims=True), new)
            p = jnp.exp(s - m)
            pn = jnp.exp(new - m)
            den = jnp.sum(p, axis=-1, keepdims=True) + pn
            pbuf[par, t] = p
            stat[par, 0, t] = jnp.broadcast_to(pn, (8, 128))
            stat[par, 1, t] = jnp.broadcast_to(den, (8, 128))

    def values(l, c):
        s_ = slot_of(l, c)
        par = lax.rem(c, 2)
        for t in range(CHUNK):
            b = c * CHUNK + t
            p = pbuf[par, t].astype(BF16)
            o = lax.dot_general(p, vbuf[s_, t], NT, preferred_element_type=F32)
            o = o + stat[par, 0, t] * vn[pl.ds(b, 1), :]
            os_[pl.ds(b * 8, 8), :] = o / stat[par, 1, t]

    low_q = lax.broadcasted_iota(jnp.int32, (QR, 128), 1) < 64

    def remote1o(q):
        rows = pl.ds(q * QR, QR)
        blocks = pl.ds((1 - core) * 4, 4)
        return remote(to.at[blocks, rows], r1o.at[:, rows], s1o.at[q], a1o.at[q], partner)

    def remote2o(q):
        rows = pl.ds(q * QR, QR)
        return remote(co.at[:, rows], r2o.at[:, rows], s2o.at[q], a2o.at[q], across)

    def remote3o(q):
        rows = pl.ds(q * QR, QR)
        blocks = pl.ds(core * 4, 4)
        return remote(hb.at[blocks, rows], hb.at[blocks, rows], s3o.at[q], a3o.at[q], partner)

    def out_proj(q):
        rows = pl.ds(q * QR, QR)
        pairs = []
        for j in range(2):
            for pr in range(2):
                h = 4 * j + 2 * pr
                e = os_[pl.ds(q * (QR * 8) + h, QR, stride=HEADS), :]
                o = os_[pl.ds(q * (QR * 8) + h + 1, QR, stride=HEADS), :]
                if j == 0:
                    pairs.append(jnp.where(low_q, e, pltpu.roll(o, 64, 1)).astype(BF16))
                else:
                    pairs.append(jnp.where(low_q, pltpu.roll(e, 64, 1), o).astype(BF16))
        att = jnp.concatenate(pairs, axis=1)
        for nb in range(4):
            z = _dot(att, wo[:, nb * 512:(nb + 1) * 512]).astype(BF16)
            to[2 * nb, rows, :] = z[:, :CB]
            to[2 * nb + 1, rows, :] = z[:, CB:]
        remote1o(q).start()

    def chip_sum_o(q):
        rows = pl.ds(q * QR, QR)
        remote1o(q).wait_recv()
        for i in range(4):
            co[i, rows, :] = (to[core * 4 + i, rows, :].astype(F32) + r1o[i, rows, :].astype(F32)).astype(BF16)
        remote2o(q).start()

    def group_sum_o(q):
        rows = pl.ds(q * QR, QR)
        remote2o(q).wait_recv()
        for i in range(4):
            z = co[i, rows, :].astype(F32) + r2o[i, rows, :].astype(F32)
            hb[core * 4 + i, rows, :] = (xb[core * 4 + i, rows, :].astype(F32) + z).astype(BF16)
        remote3o(q).start()

    def finish_o(q, l):
        remote3o(q).wait_recv()
        norm_rows(hb, q * QR, g_mlp, l)

    def remote1m(i):
        return remote(tm.at[(1 - core) * 4 + i], r1m.at[i], s1m.at[i], a1m.at[i], partner)

    def remote2m(i):
        return remote(cm.at[i], r2m.at[i], s2m.at[i], a2m.at[i], across)

    def remote3m(i):
        return remote(xb.at[core * 4 + i], xb.at[core * 4 + i], s3m.at[i], a3m.at[i], partner)

    for i in range(NCB):
        xcopy(i).wait()

    for l in range(LAYERS):
        lead = LEAD[l]

        @pl.loop(0, NQ)
        def _(q):
            norm_rows(xb, pl.multiple_of(q * QR, QR), g_attn, l)

        project(l)
        if l == 0:
            pl.semaphore_wait(barrier, 2)

        def refill(i):
            @pl.when(i + lead < NCH)
            def _():
                kcopy(l, i + lead).start()

            @pl.when(jnp.logical_and(i >= 1, i - 1 + lead < NCH))
            def _():
                vcopy(l, i - 1 + lead).start()
            t = i + lead - NCH

            @pl.when(jnp.logical_and(t >= 0, t < 4))
            def _():
                gcopy(l, t).start()
                ucopy(l, t).start()

            @pl.when(jnp.logical_and(t >= 4, t < 8))
            def _():
                dcopy(l, t - 4).start()
                dcopy(l, t).start()

        kcopy(l, 0).wait()
        scores(l, 0)
        refill(0)

        @pl.loop(1, NCH)
        def _(i):
            vcopy(l, i - 1).wait()
            kcopy(l, i).wait()
            values(l, i - 1)
            scores(l, i)
            refill(i)
            ph = lax.rem(i, 4)

            @pl.when(ph == 0)
            def _():
                @pl.when(i == 4)
                def _():
                    for j in range(2):
                        ocopy(l, j).wait()
                out_proj(i // 4 - 1)

            @pl.when(jnp.logical_and(ph == 2, i >= 6))
            def _():
                chip_sum_o((i - 6) // 4)

            @pl.when(jnp.logical_and(ph == 3, i >= 11))
            def _():
                group_sum_o((i - 11) // 4)

        vcopy(l, NCH - 1).wait()
        values(l, NCH - 1)
        for t in range(lead, 8):
            dcopy(l, t - 4).start()
            dcopy(l, t).start()
        out_proj(3)
        group_sum_o(2)
        finish_o(0, l)
        finish_o(1, l)
        chip_sum_o(3)
        finish_o(2, l)
        group_sum_o(3)
        finish_o(3, l)
        for q in range(NQ):
            remote1o(q).wait_send()
            remote2o(q).wait_send()
            remote3o(q).wait_send()

        if l + 1 < LAYERS:
            for i in range(4):
                qcopy(l + 1, i).start()
            for i in range(2):
                ocopy(l + 1, i).start()
            for c in range(LEAD[l + 1]):
                kcopy(l + 1, c).start()
                vcopy(l + 1, c).start()

        @pl.loop(0, 4)
        def _(n):
            gcopy(l, n).wait()
            ucopy(l, n).wait()
            gate = _dot(an[...], wg[n])
            up = _dot(an[...], wu[n])
            act[:, pl.ds(pl.multiple_of(n * 512, 512), 512)] = (jax.nn.silu(gate) * up).astype(BF16)

        @pl.loop(0, 4)
        def _(i):
            theirs, mine = (1 - core) * 4 + i, core * 4 + i
            dcopy(l, theirs).wait()
            dcopy(l, mine).wait()
            tm[theirs] = _dot(act[...], wd[theirs]).astype(BF16)
            tm[mine] = _dot(act[...], wd[mine]).astype(BF16)
            remote1m(i).start()

        @pl.loop(0, 4)
        def _(i):
            remote1m(i).wait_recv()
            cm[i] = (tm[core * 4 + i].astype(F32) + r1m[i].astype(F32)).astype(BF16)
            remote2m(i).start()

        @pl.loop(0, 4)
        def _(i):
            remote2m(i).wait_recv()
            z = cm[i].astype(F32) + r2m[i].astype(F32)
            xb[core * 4 + i] = (hb[core * 4 + i].astype(F32) + z).astype(BF16)
            remote3m(i).start()
            if l + 1 == LAYERS:
                ycopy(core * 4 + i).start()

        @pl.loop(0, 4)
        def _(i):
            remote3m(i).wait_recv()
            if l + 1 == LAYERS:
                ycopy((1 - core) * 4 + i).start()

        for i in range(4):
            remote1m(i).wait_send()
            remote2m(i).wait_send()
            remote3m(i).wait_send()

    for i in range(NCB):
        ycopy(i).wait()


def solution(mesh):
    half = HD // 2
    freq = np.float32(ROPE_THETA) ** (-np.arange(half, dtype=np.float32) * np.float32(2.0) / np.float32(HD))
    freq = np.tile(freq.astype(np.float32), 4)[None, :]

    def body(x, g_attn, w_qkv, w_o, g_mlp, w_gate, w_up, w_down, k_cache, v_cache, lengths):
        kt = jnp.transpose(k_cache, (0, 1, 3, 4, 2)).reshape(LAYERS, ROWS, 2 * HD, SEQ)
        vt = jnp.transpose(v_cache, (0, 1, 3, 4, 2)).reshape(LAYERS, ROWS, 2 * HD, SEQ)
        vm, hbm, sm = (pl.BlockSpec(memory_space=s) for s in (pltpu.VMEM, pl.ANY, pltpu.SMEM))
        V, DMA = pltpu.VMEM, pltpu.SemaphoreType.DMA
        scratch = [
            V((RING, CHUNK, 2 * HD, SEQ), BF16), V((RING, CHUNK, 2 * HD, SEQ), BF16),
            V((D, QKVL), BF16), V((512, D), BF16), V((4, D, 512), BF16), V((4, D, 512), BF16), V((NCB, FFL, CB), BF16),
            V((NCB, ROWS, CB), BF16), V((NCB, ROWS, CB), BF16), V((ROWS, D), BF16), V((ROWS, FFL), BF16),
            V((NCB, ROWS, CB), BF16), V((NCB, ROWS, CB), BF16),
            V((4, ROWS, CB), BF16), V((4, ROWS, CB), BF16), V((4, ROWS, CB), BF16), V((4, ROWS, CB), BF16),
            V((4, ROWS, CB), BF16), V((4, ROWS, CB), BF16),
            V((6, ROWS, 128), F32), V((ROWS * HEADS, 128), F32), V((ROWS * HEADS, 128), F32),
            V((ROWS, 128), F32), V((ROWS, 128), F32), V((ROWS, 128), F32), V((ROWS, 128), F32),
            V((2, CHUNK, 8, SEQ), F32), V((2, 2, CHUNK, 8, 128), F32),
            DMA((RING,)), DMA((RING,)), DMA((4,)), DMA((2,)), DMA((4,)), DMA((4,)), DMA((NCB,)), DMA((NCB,)),
            DMA((NCB,)),
        ] + [DMA((4,)) for _ in range(12)]
        return pl.pallas_call(
            _kernel,
            out_shape=jax.ShapeDtypeStruct((ROWS, D), BF16),
            in_specs=[sm, vm, vm, vm, vm] + [hbm] * 8,
            out_specs=hbm,
            scratch_shapes=scratch,
            compiler_params=pltpu.CompilerParams(collective_id=0, has_side_effects=True,
                                                 vmem_limit_bytes=67043328),
            name="decoder",
        )(lengths, lengths.reshape(1, ROWS), jnp.asarray(freq), g_attn, g_mlp, x, w_qkv, w_o, w_gate, w_up, w_down,
          kt, vt)

    col = P(None, None, 'tp')
    row = P(None, 'tp', None)
    cache = P(None, 'dp', None, 'tp', None)
    return jax.shard_map(body, mesh=mesh,
                         in_specs=(P('dp', None), P(), col, row, P(), col, col, row, cache, cache, P('dp')),
                         out_specs=P('dp', None), check_vma=False)
```

```python
import functools

import jax
import jax.numpy as jnp
import numpy as np
from jax import lax
from jax.experimental import pallas as pl
from jax.experimental.pallas import tpu as pltpu
from jax.sharding import PartitionSpec as P

EPS = 1e-5
ROPE_THETA = 500000.0
MESH = pl.DeviceIdType.MESH
F32, BF16 = jnp.float32, jnp.bfloat16

LAYERS, ROWS, D, SEQ, HD = 2, 128, 2048, 512, 64
QKVL, FFL, HEADS = 768, 2048, 8
CB, NCB = 256, 8
CHUNK, NCH = 16, 8
RING = 6
LEAD = (3, RING)
GV = 4
QR, NQ = 32, 4
HR = 64
SCALE = HD ** -0.5
NT = (((1,), (1,)), ((), ()))


def _dot(a, b):
    return jnp.dot(a, b, preferred_element_type=F32)


def _kernel(lens, lenv, inv, g_attn, g_mlp, x_hbm, wqkv_hbm, wo_hbm, wg_hbm, wu_hbm, wd_hbm, k_hbm, v_hbm,
            out_hbm,
            kbuf, vbuf, wqkv, wo, wg, wu, wd, xb, hb, an, act, to, tm, r1o, r1m, co, cm, r2o, r2m,
            qkvs, qs, os_, kn, vn, cs, sn, pbuf, stat, accs,
            ksem, vsem, qsem, osem, gsem, usem, dsem, xsem, ysem,
            s1o, a1o, s2o, a2o, s3o, a3o, s1m, a1m, s2m, a2m, s3m, a3m):
    me = lax.axis_index("tp")
    core = lax.rem(me, 2)
    partner = me + 1 - 2 * core
    across = lax.rem(me + 2, 4)
    barrier = pltpu.get_barrier_semaphore()
    for dev in (partner, across):
        pl.semaphore_signal(barrier, inc=1, device_id={"tp": dev}, device_id_type=MESH)

    def slot_of(l, c):
        return lax.rem(l * NCH + c, RING)

    def kcopy(l, c):
        s = slot_of(l, c)
        return pltpu.make_async_copy(k_hbm.at[l, pl.ds(c * CHUNK, CHUNK)], kbuf.at[s], ksem.at[s])

    def vcopy(l, c):
        s = slot_of(l, c)
        return pltpu.make_async_copy(v_hbm.at[l, pl.ds(c * CHUNK * 128, CHUNK * 128)], vbuf.at[s], vsem.at[s])

    def qcopy(l, i):
        r = pl.ds(i * 512, 512)
        return pltpu.make_async_copy(wqkv_hbm.at[l, r], wqkv.at[r], qsem.at[i])

    def ocopy(l, i):
        r = pl.ds(i * 256, 256)
        return pltpu.make_async_copy(wo_hbm.at[l, r], wo.at[r], osem.at[i])

    def gcopy(l, i):
        return pltpu.make_async_copy(wg_hbm.at[l, :, pl.ds(i * 512, 512)], wg.at[i], gsem.at[i])

    def ucopy(l, i):
        return pltpu.make_async_copy(wu_hbm.at[l, :, pl.ds(i * 512, 512)], wu.at[i], usem.at[i])

    def dcopy(l, i):
        return pltpu.make_async_copy(wd_hbm.at[l, :, pl.ds(i * CB, CB)], wd.at[i], dsem.at[i])

    def xcopy(i):
        return pltpu.make_async_copy(x_hbm.at[:, pl.ds(i * CB, CB)], xb.at[i], xsem.at[i])

    def ycopy(i, hf):
        rows = pl.ds(hf * HR, HR)
        return pltpu.make_async_copy(xb.at[i, rows], out_hbm.at[rows, pl.ds(i * CB, CB)], ysem.at[hf, i])

    def remote(src, dst, send, recv, dev):
        return pltpu.make_async_remote_copy(src_ref=src, dst_ref=dst, send_sem=send, recv_sem=recv,
                                            device_id={"tp": dev}, device_id_type=MESH)

    for i in range(NCB):
        xcopy(i).start()
    for i in range(4):
        qcopy(0, i).start()
    for c in range(LEAD[0]):
        kcopy(0, c).start()
        vcopy(0, c).start()
        if c == 0:
            for i in range(2):
                ocopy(0, i).start()

    lane = lax.broadcasted_iota(jnp.int32, (ROWS, 128), 1)
    first = lax.rem(lane, 64) < 32
    token = lax.shift_right_logical(lane, 3)

    pos = jnp.transpose(jnp.broadcast_to(lenv[...].astype(F32), (ROWS, 128)))
    ang = pos * inv[...]
    cs[...] = jnp.cos(ang)
    sn[...] = jnp.where(first, -jnp.sin(ang), jnp.sin(ang))

    def norm_rows(src, r0, g_ref, l):
        rows = pl.ds(r0, QR)
        ss = jnp.zeros((QR, CB), F32)
        for kb in range(NCB):
            v = src[kb, rows, :].astype(F32)
            ss = ss + v * v
        r = lax.rsqrt(jnp.sum(ss, axis=-1, keepdims=True) * (1.0 / D) + EPS)
        for kb in range(NCB):
            v = src[kb, rows, :].astype(F32)
            g = g_ref[l:l + 1, kb * CB:(kb + 1) * CB].astype(F32)
            an[rows, kb * CB:(kb + 1) * CB] = (v * r * g).astype(BF16)

    def project(l, r0, nr):
        rows = pl.ds(r0, nr)
        low = lane[:nr] < 64
        fst = first[:nr]

        def rope(t):
            other = jnp.where(fst, pltpu.roll(t, 96, 1), pltpu.roll(t, 32, 1))
            return (t * cs[rows, :] + other * sn[rows, :]).astype(BF16).astype(F32)

        for nb in range(3):
            z = _dot(an[rows, :], wqkv[:, nb * 256:(nb + 1) * 256]).astype(BF16).astype(F32)
            qkvs[2 * nb, rows, :] = z[:, :128]
            qkvs[2 * nb + 1, rows, :] = z[:, 128:]
        for j in range(2):
            for pr in range(2):
                t = rope(qkvs[3 * j + pr, rows, :])
                swapped = pltpu.roll(t, 64, 1)
                h = 4 * j + 2 * pr
                if j == 0:
                    even, odd = jnp.where(low, t, 0.0), jnp.where(low, swapped, 0.0)
                else:
                    even, odd = jnp.where(low, 0.0, swapped), jnp.where(low, 0.0, t)
                qs[pl.ds(r0 * HEADS + h, nr, stride=HEADS), :] = even
                qs[pl.ds(r0 * HEADS + h + 1, nr, stride=HEADS), :] = odd
        k0, k1 = rope(qkvs[2, rows, :]), rope(qkvs[5, rows, :])
        kn[rows, :] = jnp.where(low, k0, pltpu.roll(k1, 64, 1))
        vn[rows, :] = jnp.where(low, pltpu.roll(qkvs[2, rows, :], 64, 1), qkvs[5, rows, :])

    pos_s = lax.broadcasted_iota(jnp.int32, (8, SEQ), 1)

    def scores(l, c):
        s_ = slot_of(l, c)
        par, par4 = lax.rem(c, 2), lax.rem(c, 4)
        for t2 in range(CHUNK // 2):
            ps = []
            for t in (2 * t2, 2 * t2 + 1):
                b = c * CHUNK + t
                q = qs[pl.ds(b * 8, 8), :]
                new = jnp.sum(q * kn[pl.ds(b, 1), :], axis=-1, keepdims=True) * SCALE
                s = _dot(q.astype(BF16), kbuf[s_, t]) * SCALE
                s = jnp.where(pos_s < lens[b], s, -jnp.inf)
                m = jnp.maximum(jnp.max(s, axis=-1, keepdims=True), new)
                p = jnp.exp(s - m)
                pn = jnp.exp(new - m)
                den = jnp.sum(p, axis=-1, keepdims=True) + pn
                ps.append(p)
                stat[par4, 0, t * 8:(t + 1) * 8, :] = jnp.broadcast_to(pn, (8, 128))
                stat[par4, 1, t * 8:(t + 1) * 8, :] = jnp.broadcast_to(den, (8, 128))
            pbuf[par, t2 * 16:(t2 + 1) * 16, :] = jnp.concatenate(ps, axis=0).astype(BF16)

    def values(l, c):
        s_ = slot_of(l, c)
        par = lax.rem(c, 2)
        p = pbuf[par]
        acc = None
        for g in range(CHUNK // GV):
            res = lax.dot_general(vbuf[s_, g * GV * 128:(g + 1) * GV * 128, :], p, NT, preferred_element_type=F32)
            for t in range(GV):
                r = res[t * 128:(t + 1) * 128]
                acc = r if acc is None else jnp.where(token == g * GV + t, r, acc)
        accs[par] = acc

    def normalise(c, row):
        par, par4 = lax.rem(c, 2), lax.rem(c, 4)
        o = jnp.transpose(accs[par])
        v = jnp.concatenate([jnp.broadcast_to(vn[pl.ds(c * CHUNK + t, 1), :], (8, 128)) for t in range(CHUNK)], axis=0)
        os_[row:row + 128, :] = (o + stat[par4, 0] * v) / stat[par4, 1]

    low_q = lax.broadcasted_iota(jnp.int32, (QR, 128), 1) < 64

    def remote1o(q):
        rows = pl.ds(q * QR, QR)
        blocks = pl.ds((1 - core) * 4, 4)
        return remote(to.at[blocks, rows], r1o.at[:, rows], s1o.at[q], a1o.at[q], partner)

    def remote2o(q):
        rows = pl.ds(q * QR, QR)
        return remote(co.at[:, rows], r2o.at[:, rows], s2o.at[q], a2o.at[q], across)

    def remote3o(q):
        rows = pl.ds(q * QR, QR)
        blocks = pl.ds(core * 4, 4)
        return remote(hb.at[blocks, rows], hb.at[blocks, rows], s3o.at[q], a3o.at[q], partner)

    def out_proj(q):
        rows = pl.ds(q * QR, QR)
        normalise(2 * q, 0)
        normalise(2 * q + 1, 128)
        pairs = []
        for j in range(2):
            for pr in range(2):
                h = 4 * j + 2 * pr
                e = os_[pl.ds(h, QR, stride=HEADS), :]
                o = os_[pl.ds(h + 1, QR, stride=HEADS), :]
                if j == 0:
                    pairs.append(jnp.where(low_q, e, pltpu.roll(o, 64, 1)).astype(BF16))
                else:
                    pairs.append(jnp.where(low_q, pltpu.roll(e, 64, 1), o).astype(BF16))
        att = jnp.concatenate(pairs, axis=1)
        for nb in range(4):
            z = _dot(att, wo[:, nb * 512:(nb + 1) * 512]).astype(BF16)
            to[2 * nb, rows, :] = z[:, :CB]
            to[2 * nb + 1, rows, :] = z[:, CB:]
        remote1o(q).start()

    def chip_sum_o(q):
        rows = pl.ds(q * QR, QR)
        remote1o(q).wait_recv()
        for i in range(4):
            co[i, rows, :] = (to[core * 4 + i, rows, :].astype(F32) + r1o[i, rows, :].astype(F32)).astype(BF16)
        remote2o(q).start()

    def group_sum_o(q):
        rows = pl.ds(q * QR, QR)
        remote2o(q).wait_recv()
        for i in range(4):
            z = co[i, rows, :].astype(F32) + r2o[i, rows, :].astype(F32)
            hb[core * 4 + i, rows, :] = (xb[core * 4 + i, rows, :].astype(F32) + z).astype(BF16)
        remote3o(q).start()

    def finish_o(q, l):
        remote3o(q).wait_recv()
        norm_rows(hb, q * QR, g_mlp, l)

    def remote1m(hf, i):
        rows = pl.ds(hf * HR, HR)
        return remote(tm.at[(1 - core) * 4 + i, rows], r1m.at[i, rows], s1m.at[hf, i], a1m.at[hf, i], partner)

    def remote2m(hf, i):
        rows = pl.ds(hf * HR, HR)
        return remote(cm.at[i, rows], r2m.at[i, rows], s2m.at[hf, i], a2m.at[hf, i], across)

    def remote3m(hf, i):
        rows = pl.ds(hf * HR, HR)
        return remote(xb.at[core * 4 + i, rows], xb.at[core * 4 + i, rows], s3m.at[hf, i], a3m.at[hf, i], partner)

    def chip_sum_m(hf):
        rows = pl.ds(hf * HR, HR)
        for i in range(4):
            remote1m(hf, i).wait_recv()
            cm[i, rows, :] = (tm[core * 4 + i, rows, :].astype(F32) + r1m[i, rows, :].astype(F32)).astype(BF16)
            remote2m(hf, i).start()

    def group_sum_m(hf, last):
        rows = pl.ds(hf * HR, HR)
        for i in range(4):
            remote2m(hf, i).wait_recv()
            z = cm[i, rows, :].astype(F32) + r2m[i, rows, :].astype(F32)
            xb[core * 4 + i, rows, :] = (hb[core * 4 + i, rows, :].astype(F32) + z).astype(BF16)
            remote3m(hf, i).start()
            if last:
                ycopy(core * 4 + i, hf).start()

    def finish_m(hf, last):
        for i in range(4):
            remote3m(hf, i).wait_recv()
            if last:
                ycopy((1 - core) * 4 + i, hf).start()

    def drain_o():
        for q in range(NQ):
            remote1o(q).wait_send()
            remote2o(q).wait_send()
            remote3o(q).wait_send()

    def drain_m(hf):
        for i in range(4):
            remote1m(hf, i).wait_send()
            remote2m(hf, i).wait_send()
            remote3m(hf, i).wait_send()

    def mlp(l, hf, hooks):
        rows = pl.ds(hf * HR, HR)
        for n in range(4):
            if hf == 0:
                gcopy(l, n).wait()
                ucopy(l, n).wait()
            gate = _dot(an[rows, :], wg[n])
            up = _dot(an[rows, :], wu[n])
            act[rows, n * 512:(n + 1) * 512] = (jax.nn.silu(gate) * up).astype(BF16)
            for f in hooks.get(n, ()):
                f()
        for i in range(4):
            theirs, mine = (1 - core) * 4 + i, core * 4 + i
            if hf == 0:
                dcopy(l, theirs).wait()
                dcopy(l, mine).wait()
            tm[theirs, rows, :] = _dot(act[rows, :], wd[theirs]).astype(BF16)
            tm[mine, rows, :] = _dot(act[rows, :], wd[mine]).astype(BF16)
            remote1m(hf, i).start()
            for f in hooks.get(4 + i, ()):
                f()

    for i in range(NCB):
        xcopy(i).wait()

    for l in range(LAYERS):
        lead = LEAD[l]
        last = l + 1 == LAYERS

        def refill(i):
            @pl.when(i + lead < NCH)
            def _():
                kcopy(l, i + lead).start()

            @pl.when(jnp.logical_and(i >= 1, i - 1 + lead < NCH))
            def _():
                vcopy(l, i - 1 + lead).start()
            t = i + lead - NCH

            @pl.when(jnp.logical_and(t >= 0, t < 2))
            def _():
                for u in range(2):
                    gcopy(l, 2 * t + u).start()
                    ucopy(l, 2 * t + u).start()

            @pl.when(jnp.logical_and(t >= 2, t < 4))
            def _():
                for u in range(2):
                    dcopy(l, 2 * (t - 2) + u).start()
                    dcopy(l, 2 * (t - 2) + u + 4).start()

        def step(i):
            vcopy(l, i - 1).wait()
            kcopy(l, i).wait()
            scores(l, i)
            values(l, i - 1)
            refill(i)

        @pl.loop(0, NQ if l == 0 else NQ // 2)
        def _(q):
            norm_rows(xb, pl.multiple_of(q * QR, QR), g_attn, l)

        for i in range(4):
            qcopy(l, i).wait()
        project(l, 0, ROWS if l == 0 else HR)
        if l == 0:
            pl.semaphore_wait(barrier, 2)
        kcopy(l, 0).wait()
        scores(l, 0)
        refill(0)

        @pl.loop(1, 4)
        def _(i):
            step(i)

            @pl.when(i == 2)
            def _():
                for j in range(2):
                    ocopy(l, j).wait()
                out_proj(0)

            @pl.when(i == 3)
            def _():
                chip_sum_o(0)
            if l > 0:
                @pl.when(i == 1)
                def _():
                    group_sum_m(1, False)

        if l > 0:
            finish_m(1, False)
            drain_m(1)

            @pl.loop(NQ // 2, NQ)
            def _(q):
                norm_rows(xb, pl.multiple_of(q * QR, QR), g_attn, l)
            project(l, HR, HR)

        @pl.loop(4, NCH)
        def _(i):
            step(i)

            @pl.when(lax.rem(i, 2) == 0)
            def _():
                out_proj(i // 2 - 1)

            @pl.when(lax.rem(i, 2) == 1)
            def _():
                chip_sum_o((i - 3) // 2)

            @pl.when(i == 6)
            def _():
                group_sum_o(0)

        vcopy(l, NCH - 1).wait()
        values(l, NCH - 1)
        for t in range(max(0, lead), 4):
            for u in range(2):
                dcopy(l, 2 * (t - 2) + u).start()
                dcopy(l, 2 * (t - 2) + u + 4).start()
        if not last:
            for i in range(4):
                qcopy(l + 1, i).start()
        out_proj(3)
        group_sum_o(1)
        finish_o(0, l)
        finish_o(1, l)
        if not last:
            for i in range(2):
                ocopy(l + 1, i).start()
            for c in range(LEAD[l + 1]):
                kcopy(l + 1, c).start()
                vcopy(l + 1, c).start()
        mlp(l, 0, {0: (lambda: chip_sum_o(3),), 1: (lambda: group_sum_o(2),)})
        group_sum_o(3)
        finish_o(2, l)
        finish_o(3, l)
        mlp(l, 1, {0: (lambda: chip_sum_m(0),)})
        chip_sum_m(1)
        drain_o()
        group_sum_m(0, last)
        finish_m(0, last)
        drain_m(0)
        if last:
            group_sum_m(1, last)
            finish_m(1, last)
            drain_m(1)

    for i in range(NCB):
        for hf in range(2):
            ycopy(i, hf).wait()


def solution(mesh):
    half = HD // 2
    freq = np.float32(ROPE_THETA) ** (-np.arange(half, dtype=np.float32) * np.float32(2.0) / np.float32(HD))
    freq = np.tile(freq.astype(np.float32), 4)[None, :]

    def body(x, g_attn, w_qkv, w_o, g_mlp, w_gate, w_up, w_down, k_cache, v_cache, lengths):
        kt = jnp.transpose(k_cache, (0, 1, 3, 4, 2)).reshape(LAYERS, ROWS, 2 * HD, SEQ)
        vt = jnp.transpose(v_cache, (0, 1, 3, 4, 2)).reshape(LAYERS, ROWS * 2 * HD, SEQ)
        vm, hbm, sm = (pl.BlockSpec(memory_space=s) for s in (pltpu.VMEM, pl.ANY, pltpu.SMEM))
        V, DMA = pltpu.VMEM, pltpu.SemaphoreType.DMA
        scratch = [
            V((RING, CHUNK, 2 * HD, SEQ), BF16), V((RING, CHUNK * 2 * HD, SEQ), BF16),
            V((D, QKVL), BF16), V((512, D), BF16), V((4, D, 512), BF16), V((4, D, 512), BF16), V((NCB, FFL, CB), BF16),
            V((NCB, ROWS, CB), BF16), V((NCB, ROWS, CB), BF16), V((ROWS, D), BF16), V((ROWS, FFL), BF16),
            V((NCB, ROWS, CB), BF16), V((NCB, ROWS, CB), BF16),
            V((4, ROWS, CB), BF16), V((4, ROWS, CB), BF16), V((4, ROWS, CB), BF16), V((4, ROWS, CB), BF16),
            V((4, ROWS, CB), BF16), V((4, ROWS, CB), BF16),
            V((6, ROWS, 128), F32), V((ROWS * HEADS, 128), F32), V((256, 128), F32),
            V((ROWS, 128), F32), V((ROWS, 128), F32), V((ROWS, 128), F32), V((ROWS, 128), F32),
            V((2, 128, SEQ), BF16), V((4, 2, 128, 128), F32), V((2, 128, 128), F32),
            DMA((RING,)), DMA((RING,)), DMA((4,)), DMA((2,)), DMA((4,)), DMA((4,)), DMA((NCB,)), DMA((NCB,)),
            DMA((2, NCB)),
        ] + [DMA((4,)) for _ in range(6)] + [DMA((2, 4)) for _ in range(6)]
        return pl.pallas_call(
            _kernel,
            out_shape=jax.ShapeDtypeStruct((ROWS, D), BF16),
            in_specs=[sm, vm, vm, vm, vm] + [hbm] * 8,
            out_specs=hbm,
            scratch_shapes=scratch,
            compiler_params=pltpu.CompilerParams(collective_id=0, has_side_effects=True,
                                                 vmem_limit_bytes=67043328),
            name="decoder",
        )(lengths, lengths.reshape(1, ROWS), jnp.asarray(freq), g_attn, g_mlp, x, w_qkv, w_o, w_gate, w_up, w_down,
          kt, vt)

    col = P(None, None, 'tp')
    row = P(None, 'tp', None)
    cache = P(None, 'dp', None, 'tp', None)
    return jax.shard_map(body, mesh=mesh,
                         in_specs=(P('dp', None), P(), col, row, P(), col, col, row, cache, cache, P('dp')),
                         out_specs=P('dp', None), check_vma=False)
```

```python
import functools

import jax
import jax.numpy as jnp
import numpy as np
from jax import lax
from jax.experimental import pallas as pl
from jax.experimental.pallas import tpu as pltpu
from jax.sharding import PartitionSpec as P

EPS = 1e-5
ROPE_THETA = 500000.0
MESH = pl.DeviceIdType.MESH
F32, BF16 = jnp.float32, jnp.bfloat16

LAYERS, ROWS, D, SEQ, HD = 2, 128, 2048, 512, 64
QKVL, FFL, HEADS = 768, 2048, 8
CB, NCB = 256, 8
CHUNK, NCH = 16, 8
RING = 6
LEAD = (3, RING)
QR, NQ = 32, 4
HR = 64
SCALE = HD ** -0.5
NT = (((1,), (1,)), ((), ()))


def _dot(a, b):
    return jnp.dot(a, b, preferred_element_type=F32)


def _kernel(lens, lenv, inv, g_attn, g_mlp, x_hbm, wqkv_hbm, wo_hbm, wg_hbm, wu_hbm, wd_hbm, k_hbm, v_hbm,
            out_hbm,
            kbuf, vbuf, wqkv, wo, wg, wu, wd, xb, hb, an, act, to, tm, r1o, r1m, co, cm, r2o, r2m,
            qkvs, qs, os_, kn, vn, cs, sn, pbuf, stat, accs,
            ksem, vsem, qsem, osem, gsem, usem, dsem, xsem, ysem,
            s1o, a1o, s2o, a2o, s3o, a3o, s1m, a1m, s2m, a2m, s3m, a3m):
    me = lax.axis_index("tp")
    core = lax.rem(me, 2)
    partner = me + 1 - 2 * core
    across = lax.rem(me + 2, 4)
    barrier = pltpu.get_barrier_semaphore()
    for dev in (partner, across):
        pl.semaphore_signal(barrier, inc=1, device_id={"tp": dev}, device_id_type=MESH)

    def slot_of(l, c):
        return lax.rem(l * NCH + c, RING)

    def kcopy(l, c):
        s = slot_of(l, c)
        return pltpu.make_async_copy(k_hbm.at[l, pl.ds(c * CHUNK, CHUNK)], kbuf.at[s], ksem.at[s])

    def vcopy(l, c):
        s = slot_of(l, c)
        return pltpu.make_async_copy(v_hbm.at[l, pl.ds(c * CHUNK * 128, CHUNK * 128)], vbuf.at[s], vsem.at[s])

    def qcopy(l, i):
        r = pl.ds(i * 512, 512)
        return pltpu.make_async_copy(wqkv_hbm.at[l, r], wqkv.at[r], qsem.at[i])

    def ocopy(l, i):
        r = pl.ds(i * 256, 256)
        return pltpu.make_async_copy(wo_hbm.at[l, r], wo.at[r], osem.at[i])

    def gcopy(l, i):
        return pltpu.make_async_copy(wg_hbm.at[l, :, pl.ds(i * 512, 512)], wg.at[i], gsem.at[i])

    def ucopy(l, i):
        return pltpu.make_async_copy(wu_hbm.at[l, :, pl.ds(i * 512, 512)], wu.at[i], usem.at[i])

    def dcopy(l, i):
        return pltpu.make_async_copy(wd_hbm.at[l, :, pl.ds(i * CB, CB)], wd.at[i], dsem.at[i])

    def xcopy(i):
        return pltpu.make_async_copy(x_hbm.at[:, pl.ds(i * CB, CB)], xb.at[i], xsem.at[i])

    def ycopy(i, hf):
        rows = pl.ds(hf * HR, HR)
        return pltpu.make_async_copy(xb.at[i, rows], out_hbm.at[rows, pl.ds(i * CB, CB)], ysem.at[hf, i])

    def remote(src, dst, send, recv, dev):
        return pltpu.make_async_remote_copy(src_ref=src, dst_ref=dst, send_sem=send, recv_sem=recv,
                                            device_id={"tp": dev}, device_id_type=MESH)

    for i in range(NCB):
        xcopy(i).start()
    for i in range(4):
        qcopy(0, i).start()
    for c in range(LEAD[0]):
        kcopy(0, c).start()
        vcopy(0, c).start()
        if c == 0:
            for i in range(2):
                ocopy(0, i).start()

    lane = lax.broadcasted_iota(jnp.int32, (ROWS, 128), 1)
    first = lax.rem(lane, 64) < 32

    pos = jnp.transpose(jnp.broadcast_to(lenv[...].astype(F32), (ROWS, 128)))
    ang = pos * inv[...]
    cs[...] = jnp.cos(ang)
    sn[...] = jnp.where(first, -jnp.sin(ang), jnp.sin(ang))

    def norm_rows(src, r0, g_ref, l):
        rows = pl.ds(r0, QR)
        ss = jnp.zeros((QR, CB), F32)
        for kb in range(NCB):
            v = src[kb, rows, :].astype(F32)
            ss = ss + v * v
        r = lax.rsqrt(jnp.sum(ss, axis=-1, keepdims=True) * (1.0 / D) + EPS)
        for kb in range(NCB):
            v = src[kb, rows, :].astype(F32)
            g = g_ref[l:l + 1, kb * CB:(kb + 1) * CB].astype(F32)
            an[rows, kb * CB:(kb + 1) * CB] = (v * r * g).astype(BF16)

    def project(l, r0, nr):
        rows = pl.ds(r0, nr)
        low = lane[:nr] < 64
        fst = first[:nr]

        def rope(t):
            other = jnp.where(fst, pltpu.roll(t, 96, 1), pltpu.roll(t, 32, 1))
            return (t * cs[rows, :] + other * sn[rows, :]).astype(BF16).astype(F32)

        for nb in range(3):
            z = _dot(an[rows, :], wqkv[:, nb * 256:(nb + 1) * 256]).astype(BF16).astype(F32)
            qkvs[2 * nb, rows, :] = z[:, :128]
            qkvs[2 * nb + 1, rows, :] = z[:, 128:]
        for j in range(2):
            for pr in range(2):
                t = rope(qkvs[3 * j + pr, rows, :])
                swapped = pltpu.roll(t, 64, 1)
                h = 4 * j + 2 * pr
                if j == 0:
                    even, odd = jnp.where(low, t, 0.0), jnp.where(low, swapped, 0.0)
                else:
                    even, odd = jnp.where(low, 0.0, swapped), jnp.where(low, 0.0, t)
                qs[pl.ds(r0 * HEADS + h, nr, stride=HEADS), :] = even
                qs[pl.ds(r0 * HEADS + h + 1, nr, stride=HEADS), :] = odd
        k0, k1 = rope(qkvs[2, rows, :]), rope(qkvs[5, rows, :])
        kn[rows, :] = jnp.where(low, k0, pltpu.roll(k1, 64, 1))
        vn[rows, :] = jnp.where(low, pltpu.roll(qkvs[2, rows, :], 64, 1), qkvs[5, rows, :])

    pos_s = lax.broadcasted_iota(jnp.int32, (8, SEQ), 1)

    def scores(l, c):
        s_ = slot_of(l, c)
        par, par4 = lax.rem(c, 2), lax.rem(c, 4)
        for t2 in range(CHUNK // 2):
            ps = []
            for t in (2 * t2, 2 * t2 + 1):
                b = c * CHUNK + t
                q = qs[pl.ds(b * 8, 8), :]
                new = jnp.sum(q * kn[pl.ds(b, 1), :], axis=-1, keepdims=True) * SCALE
                s = _dot(q.astype(BF16), kbuf[s_, t]) * SCALE
                s = jnp.where(pos_s < lens[b], s, -jnp.inf)
                m = jnp.maximum(jnp.max(s, axis=-1, keepdims=True), new)
                p = jnp.exp(s - m)
                pn = jnp.exp(new - m)
                den = jnp.sum(p, axis=-1, keepdims=True) + pn
                ps.append(p)
                stat[par4, 0, t * 8:(t + 1) * 8, :] = jnp.broadcast_to(pn, (8, 128))
                stat[par4, 1, t * 8:(t + 1) * 8, :] = jnp.broadcast_to(den, (8, 128))
            pbuf[par, t2 * 16:(t2 + 1) * 16, :] = jnp.concatenate(ps, axis=0).astype(BF16)

    def values(l, c):
        s_ = slot_of(l, c)
        par = lax.rem(c, 2)
        for t in range(CHUNK):
            p = pbuf[par, t * 8:(t + 1) * 8, :]
            accs[par, t * 8:(t + 1) * 8, :] = lax.dot_general(p, vbuf[s_, t * 128:(t + 1) * 128, :], NT,
                                                              preferred_element_type=F32)

    def normalise(c, row):
        par, par4 = lax.rem(c, 2), lax.rem(c, 4)
        v = jnp.concatenate([jnp.broadcast_to(vn[pl.ds(c * CHUNK + t, 1), :], (8, 128)) for t in range(CHUNK)], axis=0)
        os_[row:row + 128, :] = (accs[par] + stat[par4, 0] * v) / stat[par4, 1]

    low_q = lax.broadcasted_iota(jnp.int32, (QR, 128), 1) < 64

    def remote1o(q):
        rows = pl.ds(q * QR, QR)
        blocks = pl.ds((1 - core) * 4, 4)
        return remote(to.at[blocks, rows], r1o.at[:, rows], s1o.at[q], a1o.at[q], partner)

    def remote2o(q):
        rows = pl.ds(q * QR, QR)
        return remote(co.at[:, rows], r2o.at[:, rows], s2o.at[q], a2o.at[q], across)

    def remote3o(q):
        rows = pl.ds(q * QR, QR)
        blocks = pl.ds(core * 4, 4)
        return remote(hb.at[blocks, rows], hb.at[blocks, rows], s3o.at[q], a3o.at[q], partner)

    def out_proj(q):
        rows = pl.ds(q * QR, QR)
        normalise(2 * q, 0)
        normalise(2 * q + 1, 128)
        pairs = []
        for j in range(2):
            for pr in range(2):
                h = 4 * j + 2 * pr
                e = os_[pl.ds(h, QR, stride=HEADS), :]
                o = os_[pl.ds(h + 1, QR, stride=HEADS), :]
                if j == 0:
                    pairs.append(jnp.where(low_q, e, pltpu.roll(o, 64, 1)).astype(BF16))
                else:
                    pairs.append(jnp.where(low_q, pltpu.roll(e, 64, 1), o).astype(BF16))
        att = jnp.concatenate(pairs, axis=1)
        for nb in range(4):
            z = _dot(att, wo[:, nb * 512:(nb + 1) * 512]).astype(BF16)
            to[2 * nb, rows, :] = z[:, :CB]
            to[2 * nb + 1, rows, :] = z[:, CB:]
        remote1o(q).start()

    def chip_sum_o(q):
        rows = pl.ds(q * QR, QR)
        remote1o(q).wait_recv()
        for i in range(4):
            co[i, rows, :] = (to[core * 4 + i, rows, :].astype(F32) + r1o[i, rows, :].astype(F32)).astype(BF16)
        remote2o(q).start()

    def group_sum_o(q):
        rows = pl.ds(q * QR, QR)
        remote2o(q).wait_recv()
        for i in range(4):
            z = co[i, rows, :].astype(F32) + r2o[i, rows, :].astype(F32)
            hb[core * 4 + i, rows, :] = (xb[core * 4 + i, rows, :].astype(F32) + z).astype(BF16)
        remote3o(q).start()

    def finish_o(q, l):
        remote3o(q).wait_recv()
        norm_rows(hb, q * QR, g_mlp, l)

    def remote1m(hf, i):
        rows = pl.ds(hf * HR, HR)
        return remote(tm.at[(1 - core) * 4 + i, rows], r1m.at[i, rows], s1m.at[hf, i], a1m.at[hf, i], partner)

    def remote2m(hf, i):
        rows = pl.ds(hf * HR, HR)
        return remote(cm.at[i, rows], r2m.at[i, rows], s2m.at[hf, i], a2m.at[hf, i], across)

    def remote3m(hf, i):
        rows = pl.ds(hf * HR, HR)
        return remote(xb.at[core * 4 + i, rows], xb.at[core * 4 + i, rows], s3m.at[hf, i], a3m.at[hf, i], partner)

    def chip_sum_m(hf):
        rows = pl.ds(hf * HR, HR)
        for i in range(4):
            remote1m(hf, i).wait_recv()
            cm[i, rows, :] = (tm[core * 4 + i, rows, :].astype(F32) + r1m[i, rows, :].astype(F32)).astype(BF16)
            remote2m(hf, i).start()

    def group_sum_m(hf, last):
        rows = pl.ds(hf * HR, HR)
        for i in range(4):
            remote2m(hf, i).wait_recv()
            z = cm[i, rows, :].astype(F32) + r2m[i, rows, :].astype(F32)
            xb[core * 4 + i, rows, :] = (hb[core * 4 + i, rows, :].astype(F32) + z).astype(BF16)
            remote3m(hf, i).start()
            if last:
                ycopy(core * 4 + i, hf).start()

    def finish_m(hf, last):
        for i in range(4):
            remote3m(hf, i).wait_recv()
            if last:
                ycopy((1 - core) * 4 + i, hf).start()

    def drain_o():
        for q in range(NQ):
            remote1o(q).wait_send()
            remote2o(q).wait_send()
            remote3o(q).wait_send()

    def drain_m(hf):
        for i in range(4):
            remote1m(hf, i).wait_send()
            remote2m(hf, i).wait_send()
            remote3m(hf, i).wait_send()

    def gate_up(l, hf, steps):
        rows = pl.ds(hf * HR, HR)
        for n in steps:
            if hf == 0:
                gcopy(l, n).wait()
                ucopy(l, n).wait()
        for n in steps:
            gate = _dot(an[rows, :], wg[n])
            up = _dot(an[rows, :], wu[n])
            act[rows, n * 512:(n + 1) * 512] = (jax.nn.silu(gate) * up).astype(BF16)

    def down(l, hf):
        rows = pl.ds(hf * HR, HR)
        if hf == 0:
            for i in range(NCB):
                dcopy(l, i).wait()
        for i in range(4):
            theirs, mine = (1 - core) * 4 + i, core * 4 + i
            tm[theirs, rows, :] = _dot(act[rows, :], wd[theirs]).astype(BF16)
            tm[mine, rows, :] = _dot(act[rows, :], wd[mine]).astype(BF16)
            remote1m(hf, i).start()

    for i in range(NCB):
        xcopy(i).wait()

    for l in range(LAYERS):
        lead = LEAD[l]
        last = l + 1 == LAYERS

        def refill(i):
            @pl.when(i + lead < NCH)
            def _():
                kcopy(l, i + lead).start()

            @pl.when(jnp.logical_and(i >= 1, i - 1 + lead < NCH))
            def _():
                vcopy(l, i - 1 + lead).start()
            t = i + lead - NCH

            @pl.when(jnp.logical_and(t >= 0, t < 2))
            def _():
                for u in range(2):
                    gcopy(l, 2 * t + u).start()
                    ucopy(l, 2 * t + u).start()

            @pl.when(jnp.logical_and(t >= 2, t < 4))
            def _():
                for u in range(2):
                    dcopy(l, 2 * (t - 2) + u).start()
                    dcopy(l, 2 * (t - 2) + u + 4).start()

        def step(i):
            vcopy(l, i - 1).wait()
            kcopy(l, i).wait()
            scores(l, i)
            values(l, i - 1)
            refill(i)

        @pl.loop(0, NQ if l == 0 else NQ // 2)
        def _(q):
            norm_rows(xb, pl.multiple_of(q * QR, QR), g_attn, l)

        for i in range(4):
            qcopy(l, i).wait()
        project(l, 0, ROWS if l == 0 else HR)
        if l == 0:
            pl.semaphore_wait(barrier, 2)
        kcopy(l, 0).wait()
        scores(l, 0)
        refill(0)

        @pl.loop(1, 4)
        def _(i):
            step(i)

            @pl.when(i == 2)
            def _():
                for j in range(2):
                    ocopy(l, j).wait()
                out_proj(0)

            @pl.when(i == 3)
            def _():
                chip_sum_o(0)
            if l > 0:
                @pl.when(i == 1)
                def _():
                    group_sum_m(1, False)

        if l > 0:
            finish_m(1, False)
            drain_m(1)

            @pl.loop(NQ // 2, NQ)
            def _(q):
                norm_rows(xb, pl.multiple_of(q * QR, QR), g_attn, l)
            project(l, HR, HR)

        @pl.loop(4, NCH)
        def _(i):
            step(i)

            @pl.when(lax.rem(i, 2) == 0)
            def _():
                out_proj(i // 2 - 1)

            @pl.when(lax.rem(i, 2) == 1)
            def _():
                chip_sum_o((i - 3) // 2)

            @pl.when(i == 6)
            def _():
                group_sum_o(0)

        vcopy(l, NCH - 1).wait()
        values(l, NCH - 1)
        for t in range(max(0, lead), 4):
            for u in range(2):
                dcopy(l, 2 * (t - 2) + u).start()
                dcopy(l, 2 * (t - 2) + u + 4).start()
        if not last:
            for i in range(4):
                qcopy(l + 1, i).start()
        out_proj(3)
        group_sum_o(1)
        finish_o(0, l)
        finish_o(1, l)
        if not last:
            for i in range(2):
                ocopy(l + 1, i).start()
            for c in range(LEAD[l + 1]):
                kcopy(l + 1, c).start()
                vcopy(l + 1, c).start()
        gate_up(l, 0, (0,))
        chip_sum_o(3)
        gate_up(l, 0, (1, 2, 3))
        group_sum_o(2)
        down(l, 0)
        group_sum_o(3)
        finish_o(2, l)
        finish_o(3, l)
        chip_sum_m(0)
        gate_up(l, 1, range(4))
        down(l, 1)
        chip_sum_m(1)
        drain_o()
        group_sum_m(0, last)
        finish_m(0, last)
        drain_m(0)
        if last:
            group_sum_m(1, last)
            finish_m(1, last)
            drain_m(1)

    for i in range(NCB):
        for hf in range(2):
            ycopy(i, hf).wait()


def solution(mesh):
    half = HD // 2
    freq = np.float32(ROPE_THETA) ** (-np.arange(half, dtype=np.float32) * np.float32(2.0) / np.float32(HD))
    freq = np.tile(freq.astype(np.float32), 4)[None, :]

    def body(x, g_attn, w_qkv, w_o, g_mlp, w_gate, w_up, w_down, k_cache, v_cache, lengths):
        kt = jnp.transpose(k_cache, (0, 1, 3, 4, 2)).reshape(LAYERS, ROWS, 2 * HD, SEQ)
        vt = jnp.transpose(v_cache, (0, 1, 3, 4, 2)).reshape(LAYERS, ROWS * 2 * HD, SEQ)
        vm, hbm, sm = (pl.BlockSpec(memory_space=s) for s in (pltpu.VMEM, pl.ANY, pltpu.SMEM))
        V, DMA = pltpu.VMEM, pltpu.SemaphoreType.DMA
        scratch = [
            V((RING, CHUNK, 2 * HD, SEQ), BF16), V((RING, CHUNK * 2 * HD, SEQ), BF16),
            V((D, QKVL), BF16), V((512, D), BF16), V((4, D, 512), BF16), V((4, D, 512), BF16), V((NCB, FFL, CB), BF16),
            V((NCB, ROWS, CB), BF16), V((NCB, ROWS, CB), BF16), V((ROWS, D), BF16), V((ROWS, FFL), BF16),
            V((NCB, ROWS, CB), BF16), V((NCB, ROWS, CB), BF16),
            V((4, ROWS, CB), BF16), V((4, ROWS, CB), BF16), V((4, ROWS, CB), BF16), V((4, ROWS, CB), BF16),
            V((4, ROWS, CB), BF16), V((4, ROWS, CB), BF16),
            V((6, ROWS, 128), F32), V((ROWS * HEADS, 128), F32), V((256, 128), F32),
            V((ROWS, 128), F32), V((ROWS, 128), F32), V((ROWS, 128), F32), V((ROWS, 128), F32),
            V((2, 128, SEQ), BF16), V((4, 2, 128, 128), F32), V((2, 128, 128), F32),
            DMA((RING,)), DMA((RING,)), DMA((4,)), DMA((2,)), DMA((4,)), DMA((4,)), DMA((NCB,)), DMA((NCB,)),
            DMA((2, NCB)),
        ] + [DMA((4,)) for _ in range(6)] + [DMA((2, 4)) for _ in range(6)]
        return pl.pallas_call(
            _kernel,
            out_shape=jax.ShapeDtypeStruct((ROWS, D), BF16),
            in_specs=[sm, vm, vm, vm, vm] + [hbm] * 8,
            out_specs=hbm,
            scratch_shapes=scratch,
            compiler_params=pltpu.CompilerParams(collective_id=0, has_side_effects=True,
                                                 vmem_limit_bytes=67043328),
            name="decoder",
        )(lengths, lengths.reshape(1, ROWS), jnp.asarray(freq), g_attn, g_mlp, x, w_qkv, w_o, w_gate, w_up, w_down,
          kt, vt)

    col = P(None, None, 'tp')
    row = P(None, 'tp', None)
    cache = P(None, 'dp', None, 'tp', None)
    return jax.shard_map(body, mesh=mesh,
                         in_specs=(P('dp', None), P(), col, row, P(), col, col, row, cache, cache, P('dp')),
                         out_specs=P('dp', None), check_vma=False)
```

```python
import functools

import jax
import jax.numpy as jnp
import numpy as np
from jax import lax
from jax.experimental import pallas as pl
from jax.experimental.pallas import tpu as pltpu
from jax.sharding import PartitionSpec as P

EPS = 1e-5
ROPE_THETA = 500000.0
MESH = pl.DeviceIdType.MESH
F32, BF16 = jnp.float32, jnp.bfloat16

LAYERS, ROWS, D, SEQ, HD = 2, 128, 2048, 512, 64
QKVL, FFL, HEADS = 768, 2048, 8
CB, NCB = 256, 8
CHUNK, NCH = 16, 8
RING = 6
LEAD = (3, RING)
QR, NQ = 32, 4
HR = 64
VMEM_LIMIT = 64487424
SCALE = HD ** -0.5
NT = (((1,), (1,)), ((), ()))


def _dot(a, b):
    return jnp.dot(a, b, preferred_element_type=F32)


def _kernel(lens, lenv, inv, g_attn, g_mlp, x_hbm, wqkv_hbm, wo_hbm, wg_hbm, wu_hbm, wd_hbm, k_hbm, v_hbm,
            out_ref,
            kbuf, vbuf, wqkv, wo, wg, wu, wd, xb, hb, an, act, to, tm, r1o, r1m, co, cm, r2o, r2m,
            qkvs, qs, os_, kn, vn, cs, sn, pbuf, stat, accs,
            ksem, vsem, qsem, osem, gsem, usem, dsem, xsem,
            s1o, a1o, s2o, a2o, s3o, a3o, s1m, a1m, s2m, a2m, s3m, a3m):
    me = lax.axis_index("tp")
    core = lax.rem(me, 2)
    partner = me + 1 - 2 * core
    across = lax.rem(me + 2, 4)
    barrier = pltpu.get_barrier_semaphore()
    for dev in (partner, across):
        pl.semaphore_signal(barrier, inc=1, device_id={"tp": dev}, device_id_type=MESH)

    def slot_of(l, c):
        return lax.rem(l * NCH + c, RING)

    def kcopy(l, c):
        s = slot_of(l, c)
        return pltpu.make_async_copy(k_hbm.at[l, pl.ds(c * CHUNK, CHUNK)], kbuf.at[s], ksem.at[s])

    def vcopy(l, c):
        s = slot_of(l, c)
        return pltpu.make_async_copy(v_hbm.at[l, pl.ds(c * CHUNK * 128, CHUNK * 128)], vbuf.at[s], vsem.at[s])

    def qcopy(l, i):
        r = pl.ds(i * 512, 512)
        return pltpu.make_async_copy(wqkv_hbm.at[l, r], wqkv.at[r], qsem.at[i])

    def ocopy(l, i):
        r = pl.ds(i * 256, 256)
        return pltpu.make_async_copy(wo_hbm.at[l, r], wo.at[r], osem.at[i])

    def gcopy(l, i):
        return pltpu.make_async_copy(wg_hbm.at[l, :, pl.ds(i * 512, 512)], wg.at[i], gsem.at[i])

    def ucopy(l, i):
        return pltpu.make_async_copy(wu_hbm.at[l, :, pl.ds(i * 512, 512)], wu.at[i], usem.at[i])

    def dcopy(l, i):
        return pltpu.make_async_copy(wd_hbm.at[l, :, pl.ds(i * CB, CB)], wd.at[i], dsem.at[i])

    def xcopy(i):
        return pltpu.make_async_copy(x_hbm.at[:, pl.ds(i * CB, CB)], xb.at[i], xsem.at[i])

    def remote(src, dst, send, recv, dev):
        return pltpu.make_async_remote_copy(src_ref=src, dst_ref=dst, send_sem=send, recv_sem=recv,
                                            device_id={"tp": dev}, device_id_type=MESH)

    for i in range(NCB):
        xcopy(i).start()
    for i in range(4):
        qcopy(0, i).start()
    for c in range(LEAD[0]):
        kcopy(0, c).start()
        vcopy(0, c).start()
        if c == 0:
            for i in range(2):
                ocopy(0, i).start()

    lane = lax.broadcasted_iota(jnp.int32, (ROWS, 128), 1)
    first = lax.rem(lane, 64) < 32

    pos = jnp.transpose(jnp.broadcast_to(lenv[...].astype(F32), (ROWS, 128)))
    ang = pos * inv[...]
    cs[...] = jnp.cos(ang)
    sn[...] = jnp.where(first, -jnp.sin(ang), jnp.sin(ang))

    def norm_rows(src, r0, g_ref, l):
        rows = pl.ds(r0, QR)
        ss = jnp.zeros((QR, CB), F32)
        for kb in range(NCB):
            v = src[kb, rows, :].astype(F32)
            ss = ss + v * v
        r = lax.rsqrt(jnp.sum(ss, axis=-1, keepdims=True) * (1.0 / D) + EPS)
        for kb in range(NCB):
            v = src[kb, rows, :].astype(F32)
            g = g_ref[l:l + 1, kb * CB:(kb + 1) * CB].astype(F32)
            an[rows, kb * CB:(kb + 1) * CB] = (v * r * g).astype(BF16)

    def project(l, r0, nr):
        rows = pl.ds(r0, nr)
        low = lane[:nr] < 64
        fst = first[:nr]

        def rope(t):
            other = jnp.where(fst, pltpu.roll(t, 96, 1), pltpu.roll(t, 32, 1))
            return (t * cs[rows, :] + other * sn[rows, :]).astype(BF16).astype(F32)

        for nb in range(3):
            z = _dot(an[rows, :], wqkv[:, nb * 256:(nb + 1) * 256]).astype(BF16).astype(F32)
            qkvs[2 * nb, rows, :] = z[:, :128]
            qkvs[2 * nb + 1, rows, :] = z[:, 128:]
        for j in range(2):
            for pr in range(2):
                t = rope(qkvs[3 * j + pr, rows, :])
                swapped = pltpu.roll(t, 64, 1)
                h = 4 * j + 2 * pr
                if j == 0:
                    even, odd = jnp.where(low, t, 0.0), jnp.where(low, swapped, 0.0)
                else:
                    even, odd = jnp.where(low, 0.0, swapped), jnp.where(low, 0.0, t)
                qs[pl.ds(r0 * HEADS + h, nr, stride=HEADS), :] = even
                qs[pl.ds(r0 * HEADS + h + 1, nr, stride=HEADS), :] = odd
        k0, k1 = rope(qkvs[2, rows, :]), rope(qkvs[5, rows, :])
        kn[rows, :] = jnp.where(low, k0, pltpu.roll(k1, 64, 1))
        vn[rows, :] = jnp.where(low, pltpu.roll(qkvs[2, rows, :], 64, 1), qkvs[5, rows, :])

    pos_s = lax.broadcasted_iota(jnp.int32, (8, SEQ), 1)

    def scores(l, c):
        s_ = slot_of(l, c)
        par, par4 = lax.rem(c, 2), lax.rem(c, 4)
        for t2 in range(CHUNK // 2):
            ps = []
            for t in (2 * t2, 2 * t2 + 1):
                b = c * CHUNK + t
                q = qs[pl.ds(b * 8, 8), :]
                new = jnp.sum(q * kn[pl.ds(b, 1), :], axis=-1, keepdims=True) * SCALE
                s = _dot(q.astype(BF16), kbuf[s_, t]) * SCALE
                s = jnp.where(pos_s < lens[b], s, -jnp.inf)
                m = jnp.maximum(jnp.max(s, axis=-1, keepdims=True), new)
                p = jnp.exp(s - m)
                pn = jnp.exp(new - m)
                den = jnp.sum(p, axis=-1, keepdims=True) + pn
                ps.append(p)
                stat[par4, 0, t * 8:(t + 1) * 8, :] = jnp.broadcast_to(pn, (8, 128))
                stat[par4, 1, t * 8:(t + 1) * 8, :] = jnp.broadcast_to(den, (8, 128))
            pbuf[par, t2 * 16:(t2 + 1) * 16, :] = jnp.concatenate(ps, axis=0).astype(BF16)

    def values(l, c):
        s_ = slot_of(l, c)
        par = lax.rem(c, 2)
        for t in range(CHUNK):
            p = pbuf[par, t * 8:(t + 1) * 8, :]
            accs[par, t * 8:(t + 1) * 8, :] = lax.dot_general(p, vbuf[s_, t * 128:(t + 1) * 128, :], NT,
                                                              preferred_element_type=F32)

    def normalise(c, row):
        par, par4 = lax.rem(c, 2), lax.rem(c, 4)
        v = jnp.concatenate([jnp.broadcast_to(vn[pl.ds(c * CHUNK + t, 1), :], (8, 128)) for t in range(CHUNK)], axis=0)
        os_[row:row + 128, :] = (accs[par] + stat[par4, 0] * v) / stat[par4, 1]

    low_q = lax.broadcasted_iota(jnp.int32, (QR, 128), 1) < 64

    def remote1o(q):
        rows = pl.ds(q * QR, QR)
        blocks = pl.ds((1 - core) * 4, 4)
        return remote(to.at[blocks, rows], r1o.at[:, rows], s1o.at[q], a1o.at[q], partner)

    def remote2o(q):
        rows = pl.ds(q * QR, QR)
        return remote(co.at[:, rows], r2o.at[:, rows], s2o.at[q], a2o.at[q], across)

    def remote3o(q):
        rows = pl.ds(q * QR, QR)
        blocks = pl.ds(core * 4, 4)
        return remote(hb.at[blocks, rows], hb.at[blocks, rows], s3o.at[q], a3o.at[q], partner)

    def out_proj(q):
        rows = pl.ds(q * QR, QR)
        normalise(2 * q, 0)
        normalise(2 * q + 1, 128)
        pairs = []
        for j in range(2):
            for pr in range(2):
                h = 4 * j + 2 * pr
                e = os_[pl.ds(h, QR, stride=HEADS), :]
                o = os_[pl.ds(h + 1, QR, stride=HEADS), :]
                if j == 0:
                    pairs.append(jnp.where(low_q, e, pltpu.roll(o, 64, 1)).astype(BF16))
                else:
                    pairs.append(jnp.where(low_q, pltpu.roll(e, 64, 1), o).astype(BF16))
        att = jnp.concatenate(pairs, axis=1)
        for nb in range(4):
            z = _dot(att, wo[:, nb * 512:(nb + 1) * 512]).astype(BF16)
            to[2 * nb, rows, :] = z[:, :CB]
            to[2 * nb + 1, rows, :] = z[:, CB:]
        remote1o(q).start()

    def chip_sum_o(q):
        rows = pl.ds(q * QR, QR)
        remote1o(q).wait_recv()
        for i in range(4):
            co[i, rows, :] = (to[core * 4 + i, rows, :].astype(F32) + r1o[i, rows, :].astype(F32)).astype(BF16)
        remote2o(q).start()

    def group_sum_o(q):
        rows = pl.ds(q * QR, QR)
        remote2o(q).wait_recv()
        for i in range(4):
            z = co[i, rows, :].astype(F32) + r2o[i, rows, :].astype(F32)
            hb[core * 4 + i, rows, :] = (xb[core * 4 + i, rows, :].astype(F32) + z).astype(BF16)
        remote3o(q).start()

    def finish_o(q, l):
        remote3o(q).wait_recv()
        norm_rows(hb, q * QR, g_mlp, l)

    def remote1m(hf, i):
        rows = pl.ds(hf * HR, HR)
        return remote(tm.at[(1 - core) * 4 + i, rows], r1m.at[i, rows], s1m.at[hf, i], a1m.at[hf, i], partner)

    def remote2m(hf, i):
        rows = pl.ds(hf * HR, HR)
        return remote(cm.at[i, rows], r2m.at[i, rows], s2m.at[hf, i], a2m.at[hf, i], across)

    def remote3m(hf, i):
        rows = pl.ds(hf * HR, HR)
        return remote(xb.at[core * 4 + i, rows], xb.at[core * 4 + i, rows], s3m.at[hf, i], a3m.at[hf, i], partner)

    def chip_sum_m(hf, pieces):
        rows = pl.ds(hf * HR, HR)
        for i in pieces:
            remote1m(hf, i).wait_recv()
            cm[i, rows, :] = (tm[core * 4 + i, rows, :].astype(F32) + r1m[i, rows, :].astype(F32)).astype(BF16)
            remote2m(hf, i).start()

    def group_sum_m(hf, pieces):
        rows = pl.ds(hf * HR, HR)
        for i in pieces:
            remote2m(hf, i).wait_recv()
            z = cm[i, rows, :].astype(F32) + r2m[i, rows, :].astype(F32)
            xb[core * 4 + i, rows, :] = (hb[core * 4 + i, rows, :].astype(F32) + z).astype(BF16)
            remote3m(hf, i).start()

    def finish_m(hf):
        for i in range(4):
            remote3m(hf, i).wait_recv()

    def drain_o():
        for q in range(NQ):
            remote1o(q).wait_send()
            remote2o(q).wait_send()
            remote3o(q).wait_send()

    def drain_m(hf):
        for i in range(4):
            remote1m(hf, i).wait_send()
            remote2m(hf, i).wait_send()
            remote3m(hf, i).wait_send()

    def gate_up(l, hf, steps):
        rows = pl.ds(hf * HR, HR)
        for n in steps:
            if hf == 0:
                gcopy(l, n).wait()
                ucopy(l, n).wait()
        for n in steps:
            gate = _dot(an[rows, :], wg[n])
            up = _dot(an[rows, :], wu[n])
            act[rows, n * 512:(n + 1) * 512] = (jax.nn.silu(gate) * up).astype(BF16)

    def down(l, hf):
        rows = pl.ds(hf * HR, HR)
        if hf == 0:
            for i in range(NCB):
                dcopy(l, i).wait()
        for i in range(4):
            theirs, mine = (1 - core) * 4 + i, core * 4 + i
            tm[theirs, rows, :] = _dot(act[rows, :], wd[theirs]).astype(BF16)
            tm[mine, rows, :] = _dot(act[rows, :], wd[mine]).astype(BF16)
            remote1m(hf, i).start()
            if i == 2:
                chip_sum_m(hf, (0,))
        chip_sum_m(hf, (1, 2, 3))

    for i in range(NCB):
        xcopy(i).wait()

    for l in range(LAYERS):
        lead = LEAD[l]
        last = l + 1 == LAYERS

        def when(cond, f):
            if isinstance(cond, bool):
                if cond:
                    f()
            else:
                pl.when(cond)(f)

        def refill_k(c):
            when(c + lead < NCH, lambda: kcopy(l, c + lead).start())

        def refill_v(c):
            when(c + lead < NCH, lambda: vcopy(l, c + lead).start())

        def refill_w(c):
            t = c + lead - NCH

            def gate_and_up():
                for u in range(2):
                    gcopy(l, 2 * t + u).start()
                    ucopy(l, 2 * t + u).start()

            def down_pair():
                for u in range(2):
                    dcopy(l, 2 * (t - 2) + u).start()
                    dcopy(l, 2 * (t - 2) + u + 4).start()
            if isinstance(t, int):
                when(0 <= t < 2, gate_and_up)
                when(2 <= t < 4, down_pair)
            else:
                when(jnp.logical_and(t >= 0, t < 2), gate_and_up)
                when(jnp.logical_and(t >= 2, t < 4), down_pair)

        def piece(k, ahead):
            c = 2 * k
            kcopy(l, c + 1).wait()
            vcopy(l, c).wait()
            vcopy(l, c + 1).wait()
            if ahead:
                kcopy(l, c + 2).wait()
            scores(l, c + 1)
            values(l, c)
            if ahead:
                scores(l, c + 2)
            values(l, c + 1)
            out_proj(k)
            refill_k(c + 1)
            refill_v(c)
            refill_v(c + 1)
            refill_w(c + 1)
            if ahead:
                refill_k(c + 2)
                refill_w(c + 2)

        @pl.loop(0, NQ if l == 0 else NQ // 2)
        def _(q):
            norm_rows(xb, pl.multiple_of(q * QR, QR), g_attn, l)

        for i in range(4):
            qcopy(l, i).wait()
        project(l, 0, ROWS if l == 0 else HR)
        if l == 0:
            pl.semaphore_wait(barrier, 2)
        kcopy(l, 0).wait()
        scores(l, 0)
        refill_k(0)
        refill_w(0)
        for j in range(2):
            ocopy(l, j).wait()
        if l == 0:
            @pl.loop(1, NCH)
            def _(i):
                vcopy(l, i - 1).wait()
                kcopy(l, i).wait()
                scores(l, i)
                values(l, i - 1)
                refill_k(i)
                refill_v(i - 1)
                refill_w(i)

                @pl.when(jnp.logical_and(lax.rem(i, 2) == 0, i >= 2))
                def _():
                    out_proj(i // 2 - 1)

                @pl.when(jnp.logical_and(lax.rem(i, 2) == 1, i >= 3))
                def _():
                    chip_sum_o((i - 3) // 2)

                @pl.when(i == 6)
                def _():
                    group_sum_o(0)

            vcopy(l, NCH - 1).wait()
            values(l, NCH - 1)
            out_proj(3)
        else:
            piece(0, True)
            group_sum_m(1, range(4))
            piece(1, False)
            chip_sum_o(0)
            finish_m(1)
            drain_m(1)

            @pl.loop(NQ // 2, NQ)
            def _(q):
                norm_rows(xb, pl.multiple_of(q * QR, QR), g_attn, l)
            project(l, HR, HR)
            kcopy(l, 4).wait()
            scores(l, 4)
            refill_k(4)
            refill_w(4)
            chip_sum_o(1)
            piece(2, True)
            group_sum_o(0)
            piece(3, False)
            chip_sum_o(2)
        for t in range(max(0, lead), 4):
            for u in range(2):
                dcopy(l, 2 * (t - 2) + u).start()
                dcopy(l, 2 * (t - 2) + u + 4).start()
        if not last:
            for i in range(4):
                qcopy(l + 1, i).start()
        group_sum_o(1)
        finish_o(0, l)
        finish_o(1, l)
        if not last:
            for i in range(2):
                ocopy(l + 1, i).start()
            for c in range(LEAD[l + 1]):
                kcopy(l + 1, c).start()
                vcopy(l + 1, c).start()
        gate_up(l, 0, (0,))
        chip_sum_o(3)
        gate_up(l, 0, (1, 2, 3))
        group_sum_o(2)
        down(l, 0)
        group_sum_o(3)
        finish_o(2, l)
        finish_o(3, l)
        gate_up(l, 1, range(4))
        group_sum_m(0, (0,))
        down(l, 1)
        drain_o()
        group_sum_m(0, (1, 2, 3))
        finish_m(0)
        drain_m(0)
        if last:
            group_sum_m(1, range(4))
            finish_m(1)
            drain_m(1)

    for i in range(NCB):
        out_ref[:, i * CB:(i + 1) * CB] = xb[i]


def solution(mesh):
    half = HD // 2
    freq = np.float32(ROPE_THETA) ** (-np.arange(half, dtype=np.float32) * np.float32(2.0) / np.float32(HD))
    freq = np.tile(freq.astype(np.float32), 4)[None, :]

    def body(x, g_attn, w_qkv, w_o, g_mlp, w_gate, w_up, w_down, k_cache, v_cache, lengths):
        kt = jnp.transpose(k_cache, (0, 1, 3, 4, 2)).reshape(LAYERS, ROWS, 2 * HD, SEQ)
        vt = jnp.transpose(v_cache, (0, 1, 3, 4, 2)).reshape(LAYERS, ROWS * 2 * HD, SEQ)
        vm, hbm, sm = (pl.BlockSpec(memory_space=s) for s in (pltpu.VMEM, pl.ANY, pltpu.SMEM))
        V, DMA = pltpu.VMEM, pltpu.SemaphoreType.DMA
        scratch = [
            V((RING, CHUNK, 2 * HD, SEQ), BF16), V((RING, CHUNK * 2 * HD, SEQ), BF16),
            V((D, QKVL), BF16), V((512, D), BF16), V((4, D, 512), BF16), V((4, D, 512), BF16), V((NCB, FFL, CB), BF16),
            V((NCB, ROWS, CB), BF16), V((NCB, ROWS, CB), BF16), V((ROWS, D), BF16), V((ROWS, FFL), BF16),
            V((NCB, ROWS, CB), BF16), V((NCB, ROWS, CB), BF16),
            V((4, ROWS, CB), BF16), V((4, ROWS, CB), BF16), V((4, ROWS, CB), BF16), V((4, ROWS, CB), BF16),
            V((4, ROWS, CB), BF16), V((4, ROWS, CB), BF16),
            V((6, ROWS, 128), F32), V((ROWS * HEADS, 128), F32), V((256, 128), F32),
            V((ROWS, 128), F32), V((ROWS, 128), F32), V((ROWS, 128), F32), V((ROWS, 128), F32),
            V((2, 128, SEQ), BF16), V((4, 2, 128, 128), F32), V((2, 128, 128), F32),
            DMA((RING,)), DMA((RING,)), DMA((4,)), DMA((2,)), DMA((4,)), DMA((4,)), DMA((NCB,)), DMA((NCB,)),
        ] + [DMA((4,)) for _ in range(6)] + [DMA((2, 4)) for _ in range(6)]
        return pl.pallas_call(
            _kernel,
            out_shape=pltpu.VMEM((ROWS, D), BF16),
            in_specs=[sm, vm, vm, vm, vm] + [hbm] * 8,
            out_specs=vm,
            scratch_shapes=scratch,
            compiler_params=pltpu.CompilerParams(collective_id=0, has_side_effects=True,
                                                 vmem_limit_bytes=VMEM_LIMIT),
            name="decoder",
        )(lengths, lengths.reshape(1, ROWS), jnp.asarray(freq), g_attn, g_mlp, x, w_qkv, w_o, w_gate, w_up, w_down,
          kt, vt)

    col = P(None, None, 'tp')
    row = P(None, 'tp', None)
    cache = P(None, 'dp', None, 'tp', None)
    return jax.shard_map(body, mesh=mesh,
                         in_specs=(P('dp', None), P(), col, row, P(), col, col, row, cache, cache, P('dp')),
                         out_specs=P('dp', None), check_vma=False)
```

```python
import functools

import jax
import jax.numpy as jnp
import numpy as np
from jax import lax
from jax.experimental import pallas as pl
from jax.experimental.pallas import tpu as pltpu
from jax.sharding import PartitionSpec as P

EPS = 1e-5
ROPE_THETA = 500000.0
MESH = pl.DeviceIdType.MESH
F32, BF16 = jnp.float32, jnp.bfloat16

LAYERS, ROWS, D, SEQ, HD = 2, 128, 2048, 512, 64
QKVL, FFL, HEADS = 768, 2048, 8
CB, NCB = 256, 8
CHUNK, NCH = 16, 8
RING = 6
LEAD = (3, RING)
QR, NQ = 32, 4
HR = 64
VMEM_LIMIT = 64487424
SCALE = HD ** -0.5
NT = (((1,), (1,)), ((), ()))


def _dot(a, b):
    return jnp.dot(a, b, preferred_element_type=F32)


def _kernel(lens, lenv, inv, g_attn, g_mlp, x_hbm, wqkv_hbm, wo_hbm, wg_hbm, wu_hbm, wd_hbm, k_hbm, v_hbm,
            out_ref,
            kbuf, vbuf, wqkv, wo, wg, wu, wd, xb, hb, an, act, to, tm, r1o, r1m, co, cm, r2o, r2m,
            qkvs, qs, os_, kn, vn, cs, sn, pbuf, stat, accs,
            ksem, vsem, qsem, osem, gsem, usem, dsem, xsem,
            s1o, a1o, s2o, a2o, s3o, a3o, s1m, a1m, s2m, a2m, s3m, a3m):
    me = lax.axis_index("tp")
    core = lax.rem(me, 2)
    partner = me + 1 - 2 * core
    across = lax.rem(me + 2, 4)
    barrier = pltpu.get_barrier_semaphore()
    for dev in (partner, across):
        pl.semaphore_signal(barrier, inc=1, device_id={"tp": dev}, device_id_type=MESH)

    def slot_of(l, c):
        return lax.rem(l * NCH + c, RING)

    def kcopy(l, c):
        s = slot_of(l, c)
        return pltpu.make_async_copy(k_hbm.at[l, pl.ds(c * CHUNK, CHUNK)], kbuf.at[s], ksem.at[s])

    def vcopy(l, c):
        s = slot_of(l, c)
        return pltpu.make_async_copy(v_hbm.at[l, pl.ds(c * CHUNK * 128, CHUNK * 128)], vbuf.at[s], vsem.at[s])

    def qcopy(l, i):
        r = pl.ds(i * 512, 512)
        return pltpu.make_async_copy(wqkv_hbm.at[l, r], wqkv.at[r], qsem.at[i])

    def ocopy(l, i):
        r = pl.ds(i * 256, 256)
        return pltpu.make_async_copy(wo_hbm.at[l, r], wo.at[r], osem.at[i])

    def gcopy(l, i):
        return pltpu.make_async_copy(wg_hbm.at[l, :, pl.ds(i * 512, 512)], wg.at[i], gsem.at[i])

    def ucopy(l, i):
        return pltpu.make_async_copy(wu_hbm.at[l, :, pl.ds(i * 512, 512)], wu.at[i], usem.at[i])

    def dcopy(l, i):
        return pltpu.make_async_copy(wd_hbm.at[l, :, pl.ds(i * CB, CB)], wd.at[i], dsem.at[i])

    def xcopy(i):
        return pltpu.make_async_copy(x_hbm.at[:, pl.ds(i * CB, CB)], xb.at[i], xsem.at[i])

    def remote(src, dst, send, recv, dev):
        return pltpu.make_async_remote_copy(src_ref=src, dst_ref=dst, send_sem=send, recv_sem=recv,
                                            device_id={"tp": dev}, device_id_type=MESH)

    for i in range(NCB):
        xcopy(i).start()
    for i in range(4):
        qcopy(0, i).start()
    for c in range(LEAD[0]):
        kcopy(0, c).start()
        vcopy(0, c).start()
        if c == 0:
            for i in range(2):
                ocopy(0, i).start()

    lane = lax.broadcasted_iota(jnp.int32, (ROWS, 128), 1)
    first = lax.rem(lane, 64) < 32

    pos = jnp.transpose(jnp.broadcast_to(lenv[...].astype(F32), (ROWS, 128)))
    ang = pos * inv[...]
    cs[...] = jnp.cos(ang)
    sn[...] = jnp.where(first, -jnp.sin(ang), jnp.sin(ang))

    def norm_rows(src, r0, g_ref, l):
        rows = pl.ds(r0, QR)
        ss = jnp.zeros((QR, CB), F32)
        for kb in range(NCB):
            v = src[kb, rows, :].astype(F32)
            ss = ss + v * v
        r = lax.rsqrt(jnp.sum(ss, axis=-1, keepdims=True) * (1.0 / D) + EPS)
        for kb in range(NCB):
            v = src[kb, rows, :].astype(F32)
            g = g_ref[l:l + 1, kb * CB:(kb + 1) * CB].astype(F32)
            an[rows, kb * CB:(kb + 1) * CB] = (v * r * g).astype(BF16)

    def project(l, r0, nr):
        rows = pl.ds(r0, nr)
        low = lane[:nr] < 64
        fst = first[:nr]

        def rope(t):
            other = jnp.where(fst, pltpu.roll(t, 96, 1), pltpu.roll(t, 32, 1))
            return (t * cs[rows, :] + other * sn[rows, :]).astype(BF16).astype(F32)

        for nb in range(3):
            z = _dot(an[rows, :], wqkv[:, nb * 256:(nb + 1) * 256]).astype(BF16).astype(F32)
            qkvs[2 * nb, rows, :] = z[:, :128]
            qkvs[2 * nb + 1, rows, :] = z[:, 128:]
        for j in range(2):
            for pr in range(2):
                t = rope(qkvs[3 * j + pr, rows, :])
                swapped = pltpu.roll(t, 64, 1)
                h = 4 * j + 2 * pr
                if j == 0:
                    even, odd = jnp.where(low, t, 0.0), jnp.where(low, swapped, 0.0)
                else:
                    even, odd = jnp.where(low, 0.0, swapped), jnp.where(low, 0.0, t)
                qs[pl.ds(r0 * HEADS + h, nr, stride=HEADS), :] = even
                qs[pl.ds(r0 * HEADS + h + 1, nr, stride=HEADS), :] = odd
        k0, k1 = rope(qkvs[2, rows, :]), rope(qkvs[5, rows, :])
        kn[rows, :] = jnp.where(low, k0, pltpu.roll(k1, 64, 1))
        vn[rows, :] = jnp.where(low, pltpu.roll(qkvs[2, rows, :], 64, 1), qkvs[5, rows, :])

    pos_s = lax.broadcasted_iota(jnp.int32, (8, SEQ), 1)

    def scores(l, c):
        s_ = slot_of(l, c)
        par, par4 = lax.rem(c, 2), lax.rem(c, 4)
        for t2 in range(CHUNK // 2):
            ps = []
            for t in (2 * t2, 2 * t2 + 1):
                b = c * CHUNK + t
                q = qs[pl.ds(b * 8, 8), :]
                new = jnp.sum(q * kn[pl.ds(b, 1), :], axis=-1, keepdims=True) * SCALE
                s = _dot(q.astype(BF16), kbuf[s_, t]) * SCALE
                s = jnp.where(pos_s < lens[b], s, -jnp.inf)
                m = jnp.maximum(jnp.max(s, axis=-1, keepdims=True), new)
                p = jnp.exp(s - m)
                pn = jnp.exp(new - m)
                den = jnp.sum(p, axis=-1, keepdims=True) + pn
                ps.append(p)
                stat[par4, 0, t * 8:(t + 1) * 8, :] = jnp.broadcast_to(pn, (8, 128))
                stat[par4, 1, t * 8:(t + 1) * 8, :] = jnp.broadcast_to(den, (8, 128))
            pbuf[par, t2 * 16:(t2 + 1) * 16, :] = jnp.concatenate(ps, axis=0).astype(BF16)

    def values(l, c):
        s_ = slot_of(l, c)
        par = lax.rem(c, 2)
        for t in range(CHUNK):
            p = pbuf[par, t * 8:(t + 1) * 8, :]
            accs[par, t * 8:(t + 1) * 8, :] = lax.dot_general(p, vbuf[s_, t * 128:(t + 1) * 128, :], NT,
                                                              preferred_element_type=F32)

    def normalise(c, row):
        par, par4 = lax.rem(c, 2), lax.rem(c, 4)
        v = jnp.concatenate([jnp.broadcast_to(vn[pl.ds(c * CHUNK + t, 1), :], (8, 128)) for t in range(CHUNK)], axis=0)
        os_[row:row + 128, :] = (accs[par] + stat[par4, 0] * v) / stat[par4, 1]

    low_q = lax.broadcasted_iota(jnp.int32, (QR, 128), 1) < 64

    def remote1o(q):
        rows = pl.ds(q * QR, QR)
        blocks = pl.ds((1 - core) * 4, 4)
        return remote(to.at[blocks, rows], r1o.at[:, rows], s1o.at[q], a1o.at[q], partner)

    def remote2o(q):
        rows = pl.ds(q * QR, QR)
        return remote(co.at[:, rows], r2o.at[:, rows], s2o.at[q], a2o.at[q], across)

    def remote3o(q):
        rows = pl.ds(q * QR, QR)
        blocks = pl.ds(core * 4, 4)
        return remote(hb.at[blocks, rows], hb.at[blocks, rows], s3o.at[q], a3o.at[q], partner)

    def out_proj(q):
        rows = pl.ds(q * QR, QR)
        normalise(2 * q, 0)
        normalise(2 * q + 1, 128)
        pairs = []
        for j in range(2):
            for pr in range(2):
                h = 4 * j + 2 * pr
                e = os_[pl.ds(h, QR, stride=HEADS), :]
                o = os_[pl.ds(h + 1, QR, stride=HEADS), :]
                if j == 0:
                    pairs.append(jnp.where(low_q, e, pltpu.roll(o, 64, 1)).astype(BF16))
                else:
                    pairs.append(jnp.where(low_q, pltpu.roll(e, 64, 1), o).astype(BF16))
        att = jnp.concatenate(pairs, axis=1)
        for nb in range(4):
            z = _dot(att, wo[:, nb * 512:(nb + 1) * 512]).astype(BF16)
            to[2 * nb, rows, :] = z[:, :CB]
            to[2 * nb + 1, rows, :] = z[:, CB:]
        remote1o(q).start()

    def chip_sum_o(q):
        rows = pl.ds(q * QR, QR)
        remote1o(q).wait_recv()
        for i in range(4):
            co[i, rows, :] = (to[core * 4 + i, rows, :].astype(F32) + r1o[i, rows, :].astype(F32)).astype(BF16)
        remote2o(q).start()

    def group_sum_o(q):
        rows = pl.ds(q * QR, QR)
        remote2o(q).wait_recv()
        for i in range(4):
            z = co[i, rows, :].astype(F32) + r2o[i, rows, :].astype(F32)
            hb[core * 4 + i, rows, :] = (xb[core * 4 + i, rows, :].astype(F32) + z).astype(BF16)
        remote3o(q).start()

    def finish_o(q, l):
        remote3o(q).wait_recv()
        norm_rows(hb, q * QR, g_mlp, l)

    def remote1m(hf, i):
        rows = pl.ds(hf * HR, HR)
        return remote(tm.at[(1 - core) * 4 + i, rows], r1m.at[i, rows], s1m.at[hf, i], a1m.at[hf, i], partner)

    def remote2m(hf, i):
        rows = pl.ds(hf * HR, HR)
        return remote(cm.at[i, rows], r2m.at[i, rows], s2m.at[hf, i], a2m.at[hf, i], across)

    def remote3m(hf, i):
        rows = pl.ds(hf * HR, HR)
        return remote(xb.at[core * 4 + i, rows], xb.at[core * 4 + i, rows], s3m.at[hf, i], a3m.at[hf, i], partner)

    def chip_sum_m(hf, pieces):
        rows = pl.ds(hf * HR, HR)
        for i in pieces:
            remote1m(hf, i).wait_recv()
            cm[i, rows, :] = (tm[core * 4 + i, rows, :].astype(F32) + r1m[i, rows, :].astype(F32)).astype(BF16)
            remote2m(hf, i).start()

    def group_sum_m(hf, pieces):
        rows = pl.ds(hf * HR, HR)
        for i in pieces:
            remote2m(hf, i).wait_recv()
            z = cm[i, rows, :].astype(F32) + r2m[i, rows, :].astype(F32)
            xb[core * 4 + i, rows, :] = (hb[core * 4 + i, rows, :].astype(F32) + z).astype(BF16)
            remote3m(hf, i).start()

    def finish_m(hf):
        for i in range(4):
            remote3m(hf, i).wait_recv()

    def drain_o():
        for q in range(NQ):
            remote1o(q).wait_send()
            remote2o(q).wait_send()
            remote3o(q).wait_send()

    def drain_m(hf):
        for i in range(4):
            remote1m(hf, i).wait_send()
            remote2m(hf, i).wait_send()
            remote3m(hf, i).wait_send()

    def gate_up(l, hf, steps):
        rows = pl.ds(hf * HR, HR)
        for n in steps:
            if hf == 0:
                gcopy(l, n).wait()
                ucopy(l, n).wait()
        for n in steps:
            gate = _dot(an[rows, :], wg[n])
            up = _dot(an[rows, :], wu[n])
            act[rows, n * 512:(n + 1) * 512] = (jax.nn.silu(gate) * up).astype(BF16)

    def down(l, hf):
        rows = pl.ds(hf * HR, HR)
        if hf == 0:
            for i in range(NCB):
                dcopy(l, i).wait()
        for i in range(4):
            theirs, mine = (1 - core) * 4 + i, core * 4 + i
            tm[theirs, rows, :] = _dot(act[rows, :], wd[theirs]).astype(BF16)
            tm[mine, rows, :] = _dot(act[rows, :], wd[mine]).astype(BF16)
            if i % 2 == 1:
                remote1m(hf, i - 1).start()
                remote1m(hf, i).start()

    for i in range(NCB):
        xcopy(i).wait()

    for l in range(LAYERS):
        lead = LEAD[l]
        last = l + 1 == LAYERS

        def when(cond, f):
            if isinstance(cond, bool):
                if cond:
                    f()
            else:
                pl.when(cond)(f)

        def refill_k(c):
            when(c + lead < NCH, lambda: kcopy(l, c + lead).start())

        def refill_v(c):
            when(c + lead < NCH, lambda: vcopy(l, c + lead).start())

        def refill_w(c):
            t = c + lead - NCH

            def gate_and_up():
                for u in range(2):
                    gcopy(l, 2 * t + u).start()
                    ucopy(l, 2 * t + u).start()

            def down_pair():
                for u in range(2):
                    dcopy(l, 2 * (t - 2) + u).start()
                    dcopy(l, 2 * (t - 2) + u + 4).start()
            if isinstance(t, int):
                when(0 <= t < 2, gate_and_up)
                when(2 <= t < 4, down_pair)
            else:
                when(jnp.logical_and(t >= 0, t < 2), gate_and_up)
                when(jnp.logical_and(t >= 2, t < 4), down_pair)

        def piece(k, ahead):
            c = 2 * k
            kcopy(l, c + 1).wait()
            vcopy(l, c).wait()
            vcopy(l, c + 1).wait()
            if ahead:
                kcopy(l, c + 2).wait()
            scores(l, c + 1)
            values(l, c)
            if ahead:
                scores(l, c + 2)
            values(l, c + 1)
            out_proj(k)
            refill_k(c + 1)
            refill_v(c)
            refill_v(c + 1)
            refill_w(c + 1)
            if ahead:
                refill_k(c + 2)
                refill_w(c + 2)

        @pl.loop(0, NQ if l == 0 else NQ // 2)
        def _(q):
            norm_rows(xb, pl.multiple_of(q * QR, QR), g_attn, l)

        for i in range(4):
            qcopy(l, i).wait()
        project(l, 0, ROWS if l == 0 else HR)
        if l == 0:
            pl.semaphore_wait(barrier, 2)
        kcopy(l, 0).wait()
        scores(l, 0)
        refill_k(0)
        refill_w(0)
        for j in range(2):
            ocopy(l, j).wait()
        if l == 0:
            @pl.loop(1, NCH)
            def _(i):
                vcopy(l, i - 1).wait()
                kcopy(l, i).wait()
                scores(l, i)
                values(l, i - 1)
                refill_k(i)
                refill_v(i - 1)
                refill_w(i)

                @pl.when(jnp.logical_and(lax.rem(i, 2) == 0, i >= 2))
                def _():
                    out_proj(i // 2 - 1)

                @pl.when(jnp.logical_and(lax.rem(i, 2) == 1, i >= 3))
                def _():
                    chip_sum_o((i - 3) // 2)

                @pl.when(i == 6)
                def _():
                    group_sum_o(0)

            vcopy(l, NCH - 1).wait()
            values(l, NCH - 1)
            out_proj(3)
        else:
            piece(0, True)
            group_sum_m(1, range(4))
            piece(1, False)
            chip_sum_o(0)
            finish_m(1)
            drain_m(1)

            @pl.loop(NQ // 2, NQ)
            def _(q):
                norm_rows(xb, pl.multiple_of(q * QR, QR), g_attn, l)
            project(l, HR, HR)
            kcopy(l, 4).wait()
            scores(l, 4)
            refill_k(4)
            refill_w(4)
            chip_sum_o(1)
            piece(2, True)
            group_sum_o(0)
            piece(3, False)
            chip_sum_o(2)
        for t in range(max(0, lead), 4):
            for u in range(2):
                dcopy(l, 2 * (t - 2) + u).start()
                dcopy(l, 2 * (t - 2) + u + 4).start()
        if not last:
            for i in range(4):
                qcopy(l + 1, i).start()
        group_sum_o(1)
        finish_o(0, l)
        finish_o(1, l)
        if not last:
            for i in range(2):
                ocopy(l + 1, i).start()
            for c in range(LEAD[l + 1]):
                kcopy(l + 1, c).start()
                vcopy(l + 1, c).start()
        gate_up(l, 0, (0,))
        chip_sum_o(3)
        gate_up(l, 0, (1, 2, 3))
        group_sum_o(2)
        down(l, 0)
        group_sum_o(3)
        chip_sum_m(0, range(4))
        finish_o(2, l)
        finish_o(3, l)
        gate_up(l, 1, range(4))
        down(l, 1)
        drain_o()
        group_sum_m(0, range(4))
        chip_sum_m(1, range(4))
        finish_m(0)
        drain_m(0)
        if last:
            group_sum_m(1, range(4))
            finish_m(1)
            drain_m(1)

    for i in range(NCB):
        out_ref[:, i * CB:(i + 1) * CB] = xb[i]


def solution(mesh):
    half = HD // 2
    freq = np.float32(ROPE_THETA) ** (-np.arange(half, dtype=np.float32) * np.float32(2.0) / np.float32(HD))
    freq = np.tile(freq.astype(np.float32), 4)[None, :]

    def body(x, g_attn, w_qkv, w_o, g_mlp, w_gate, w_up, w_down, k_cache, v_cache, lengths):
        kt = jnp.transpose(k_cache, (0, 1, 3, 4, 2)).reshape(LAYERS, ROWS, 2 * HD, SEQ)
        vt = jnp.transpose(v_cache, (0, 1, 3, 4, 2)).reshape(LAYERS, ROWS * 2 * HD, SEQ)
        vm, hbm, sm = (pl.BlockSpec(memory_space=s) for s in (pltpu.VMEM, pl.ANY, pltpu.SMEM))
        V, DMA = pltpu.VMEM, pltpu.SemaphoreType.DMA
        scratch = [
            V((RING, CHUNK, 2 * HD, SEQ), BF16), V((RING, CHUNK * 2 * HD, SEQ), BF16),
            V((D, QKVL), BF16), V((512, D), BF16), V((4, D, 512), BF16), V((4, D, 512), BF16), V((NCB, FFL, CB), BF16),
            V((NCB, ROWS, CB), BF16), V((NCB, ROWS, CB), BF16), V((ROWS, D), BF16), V((ROWS, FFL), BF16),
            V((NCB, ROWS, CB), BF16), V((NCB, ROWS, CB), BF16),
            V((4, ROWS, CB), BF16), V((4, ROWS, CB), BF16), V((4, ROWS, CB), BF16), V((4, ROWS, CB), BF16),
            V((4, ROWS, CB), BF16), V((4, ROWS, CB), BF16),
            V((6, ROWS, 128), F32), V((ROWS * HEADS, 128), F32), V((256, 128), F32),
            V((ROWS, 128), F32), V((ROWS, 128), F32), V((ROWS, 128), F32), V((ROWS, 128), F32),
            V((2, 128, SEQ), BF16), V((4, 2, 128, 128), F32), V((2, 128, 128), F32),
            DMA((RING,)), DMA((RING,)), DMA((4,)), DMA((2,)), DMA((4,)), DMA((4,)), DMA((NCB,)), DMA((NCB,)),
        ] + [DMA((4,)) for _ in range(6)] + [DMA((2, 4)) for _ in range(6)]
        return pl.pallas_call(
            _kernel,
            out_shape=pltpu.VMEM((ROWS, D), BF16),
            in_specs=[sm, vm, vm, vm, vm] + [hbm] * 8,
            out_specs=vm,
            scratch_shapes=scratch,
            compiler_params=pltpu.CompilerParams(collective_id=0, has_side_effects=True,
                                                 vmem_limit_bytes=VMEM_LIMIT),
            name="decoder",
        )(lengths, lengths.reshape(1, ROWS), jnp.asarray(freq), g_attn, g_mlp, x, w_qkv, w_o, w_gate, w_up, w_down,
          kt, vt)

    col = P(None, None, 'tp')
    row = P(None, 'tp', None)
    cache = P(None, 'dp', None, 'tp', None)
    return jax.shard_map(body, mesh=mesh,
                         in_specs=(P('dp', None), P(), col, row, P(), col, col, row, cache, cache, P('dp')),
                         out_specs=P('dp', None), check_vma=False)
```

```python
import functools

import jax
import jax.numpy as jnp
import numpy as np
from jax import lax
from jax.experimental import pallas as pl
from jax.experimental.pallas import tpu as pltpu
from jax.sharding import PartitionSpec as P

EPS = 1e-5
ROPE_THETA = 500000.0
MESH = pl.DeviceIdType.MESH
F32, BF16 = jnp.float32, jnp.bfloat16

LAYERS, ROWS, D, SEQ, HD = 2, 128, 2048, 512, 64
QKVL, FFL, HEADS = 768, 2048, 8
CB, NCB = 256, 8
CHUNK, NCH = 16, 8
RING = 6
LEAD = (3, RING)
QR, NQ = 32, 4
HR = 64
VMEM_LIMIT = 64487424
SCALE = HD ** -0.5
NT = (((1,), (1,)), ((), ()))


def _dot(a, b):
    return jnp.dot(a, b, preferred_element_type=F32)


def _kernel(lens, lenv, inv, g_attn, g_mlp, x_hbm, wqkv_hbm, wo_hbm, wg_hbm, wu_hbm, wd_hbm, k_hbm, v_hbm,
            out_ref,
            kbuf, vbuf, wqkv, wo, wg, wu, wd, xb, hb, an, act, to, tm, r1o, r1m, co, cm, r2o, r2m,
            qkvs, qs, os_, kn, vn, cs, sn, pbuf, stat, accs,
            ksem, vsem, qsem, osem, gsem, usem, dsem, xsem,
            s1o, a1o, s2o, a2o, s3o, a3o, s1m, a1m, s2m, a2m, s3m, a3m):
    me = lax.axis_index("tp")
    core = lax.rem(me, 2)
    partner = me + 1 - 2 * core
    across = lax.rem(me + 2, 4)
    barrier = pltpu.get_barrier_semaphore()
    for dev in (partner, across):
        pl.semaphore_signal(barrier, inc=1, device_id={"tp": dev}, device_id_type=MESH)

    def slot_of(l, c):
        return lax.rem(l * NCH + c, RING)

    def kcopy(l, c):
        s = slot_of(l, c)
        return pltpu.make_async_copy(k_hbm.at[l, pl.ds(c * CHUNK, CHUNK)], kbuf.at[s], ksem.at[s])

    def vcopy(l, c):
        s = slot_of(l, c)
        return pltpu.make_async_copy(v_hbm.at[l, pl.ds(c * CHUNK * 128, CHUNK * 128)], vbuf.at[s], vsem.at[s])

    def qcopy(l, i):
        r = pl.ds(i * 512, 512)
        return pltpu.make_async_copy(wqkv_hbm.at[l, r], wqkv.at[r], qsem.at[i])

    def ocopy(l, i):
        r = pl.ds(i * 256, 256)
        return pltpu.make_async_copy(wo_hbm.at[l, r], wo.at[r], osem.at[i])

    def gcopy(l, i):
        return pltpu.make_async_copy(wg_hbm.at[l, :, pl.ds(i * 512, 512)], wg.at[i], gsem.at[i])

    def ucopy(l, i):
        return pltpu.make_async_copy(wu_hbm.at[l, :, pl.ds(i * 512, 512)], wu.at[i], usem.at[i])

    def dcopy(l, i):
        return pltpu.make_async_copy(wd_hbm.at[l, :, pl.ds(i * CB, CB)], wd.at[i], dsem.at[i])

    def xcopy(i):
        return pltpu.make_async_copy(x_hbm.at[:, pl.ds(i * CB, CB)], xb.at[i], xsem.at[i])

    def remote(src, dst, send, recv, dev):
        return pltpu.make_async_remote_copy(src_ref=src, dst_ref=dst, send_sem=send, recv_sem=recv,
                                            device_id={"tp": dev}, device_id_type=MESH)

    for i in range(NCB):
        xcopy(i).start()
    for i in range(4):
        qcopy(0, i).start()
    for c in range(LEAD[0]):
        kcopy(0, c).start()
        vcopy(0, c).start()
        if c == 0:
            for i in range(2):
                ocopy(0, i).start()

    lane = lax.broadcasted_iota(jnp.int32, (ROWS, 128), 1)
    first = lax.rem(lane, 64) < 32

    pos = jnp.transpose(jnp.broadcast_to(lenv[...].astype(F32), (ROWS, 128)))
    ang = pos * inv[...]
    cs[...] = jnp.cos(ang)
    sn[...] = jnp.where(first, -jnp.sin(ang), jnp.sin(ang))

    def norm_rows(src, r0, g_ref, l):
        rows = pl.ds(r0, QR)
        ss = jnp.zeros((QR, CB), F32)
        for kb in range(NCB):
            v = src[kb, rows, :].astype(F32)
            ss = ss + v * v
        r = lax.rsqrt(jnp.sum(ss, axis=-1, keepdims=True) * (1.0 / D) + EPS)
        for kb in range(NCB):
            v = src[kb, rows, :].astype(F32)
            g = g_ref[l:l + 1, kb * CB:(kb + 1) * CB].astype(F32)
            an[rows, kb * CB:(kb + 1) * CB] = (v * r * g).astype(BF16)

    def project(l, r0, nr):
        rows = pl.ds(r0, nr)
        low = lane[:nr] < 64
        fst = first[:nr]

        def rope(t):
            other = jnp.where(fst, pltpu.roll(t, 96, 1), pltpu.roll(t, 32, 1))
            return (t * cs[rows, :] + other * sn[rows, :]).astype(BF16).astype(F32)

        for nb in range(3):
            z = _dot(an[rows, :], wqkv[:, nb * 256:(nb + 1) * 256]).astype(BF16).astype(F32)
            qkvs[2 * nb, rows, :] = z[:, :128]
            qkvs[2 * nb + 1, rows, :] = z[:, 128:]
        for j in range(2):
            for pr in range(2):
                t = rope(qkvs[3 * j + pr, rows, :])
                swapped = pltpu.roll(t, 64, 1)
                h = 4 * j + 2 * pr
                if j == 0:
                    even, odd = jnp.where(low, t, 0.0), jnp.where(low, swapped, 0.0)
                else:
                    even, odd = jnp.where(low, 0.0, swapped), jnp.where(low, 0.0, t)
                qs[pl.ds(r0 * HEADS + h, nr, stride=HEADS), :] = even
                qs[pl.ds(r0 * HEADS + h + 1, nr, stride=HEADS), :] = odd
        k0, k1 = rope(qkvs[2, rows, :]), rope(qkvs[5, rows, :])
        kn[rows, :] = jnp.where(low, k0, pltpu.roll(k1, 64, 1))
        vn[rows, :] = jnp.where(low, pltpu.roll(qkvs[2, rows, :], 64, 1), qkvs[5, rows, :])

    pos_s = lax.broadcasted_iota(jnp.int32, (8, SEQ), 1)

    def scores(l, c):
        s_ = slot_of(l, c)
        par, par4 = lax.rem(c, 2), lax.rem(c, 4)
        for t2 in range(CHUNK // 2):
            ps = []
            for t in (2 * t2, 2 * t2 + 1):
                b = c * CHUNK + t
                q = qs[pl.ds(b * 8, 8), :]
                new = jnp.sum(q * kn[pl.ds(b, 1), :], axis=-1, keepdims=True) * SCALE
                s = _dot(q.astype(BF16), kbuf[s_, t]) * SCALE
                s = jnp.where(pos_s < lens[b], s, -jnp.inf)
                m = jnp.maximum(jnp.max(s, axis=-1, keepdims=True), new)
                p = jnp.exp(s - m)
                pn = jnp.exp(new - m)
                den = jnp.sum(p, axis=-1, keepdims=True) + pn
                ps.append(p)
                stat[par4, 0, t * 8:(t + 1) * 8, :] = jnp.broadcast_to(pn, (8, 128))
                stat[par4, 1, t * 8:(t + 1) * 8, :] = jnp.broadcast_to(den, (8, 128))
            pbuf[par, t2 * 16:(t2 + 1) * 16, :] = jnp.concatenate(ps, axis=0).astype(BF16)

    def values(l, c):
        s_ = slot_of(l, c)
        par = lax.rem(c, 2)
        for t in range(CHUNK):
            p = pbuf[par, t * 8:(t + 1) * 8, :]
            accs[par, t * 8:(t + 1) * 8, :] = lax.dot_general(p, vbuf[s_, t * 128:(t + 1) * 128, :], NT,
                                                              preferred_element_type=F32)

    def normalise(c, row):
        par, par4 = lax.rem(c, 2), lax.rem(c, 4)
        v = jnp.concatenate([jnp.broadcast_to(vn[pl.ds(c * CHUNK + t, 1), :], (8, 128)) for t in range(CHUNK)], axis=0)
        os_[row:row + 128, :] = (accs[par] + stat[par4, 0] * v) / stat[par4, 1]

    low_q = lax.broadcasted_iota(jnp.int32, (QR, 128), 1) < 64

    def remote1o(q):
        rows = pl.ds(q * QR, QR)
        blocks = pl.ds((1 - core) * 4, 4)
        return remote(to.at[blocks, rows], r1o.at[:, rows], s1o.at[q], a1o.at[q], partner)

    def remote2o(q):
        rows = pl.ds(q * QR, QR)
        return remote(co.at[:, rows], r2o.at[:, rows], s2o.at[q], a2o.at[q], across)

    def remote3o(q):
        rows = pl.ds(q * QR, QR)
        blocks = pl.ds(core * 4, 4)
        return remote(hb.at[blocks, rows], hb.at[blocks, rows], s3o.at[q], a3o.at[q], partner)

    def out_proj(q):
        rows = pl.ds(q * QR, QR)
        normalise(2 * q, 0)
        normalise(2 * q + 1, 128)
        pairs = []
        for j in range(2):
            for pr in range(2):
                h = 4 * j + 2 * pr
                e = os_[pl.ds(h, QR, stride=HEADS), :]
                o = os_[pl.ds(h + 1, QR, stride=HEADS), :]
                if j == 0:
                    pairs.append(jnp.where(low_q, e, pltpu.roll(o, 64, 1)).astype(BF16))
                else:
                    pairs.append(jnp.where(low_q, pltpu.roll(e, 64, 1), o).astype(BF16))
        att = jnp.concatenate(pairs, axis=1)
        for nb in range(4):
            z = _dot(att, wo[:, nb * 512:(nb + 1) * 512]).astype(BF16)
            to[2 * nb, rows, :] = z[:, :CB]
            to[2 * nb + 1, rows, :] = z[:, CB:]
        remote1o(q).start()

    def chip_sum_o(q):
        rows = pl.ds(q * QR, QR)
        remote1o(q).wait_recv()
        for i in range(4):
            co[i, rows, :] = (to[core * 4 + i, rows, :].astype(F32) + r1o[i, rows, :].astype(F32)).astype(BF16)
        remote2o(q).start()

    def group_sum_o(q):
        rows = pl.ds(q * QR, QR)
        remote2o(q).wait_recv()
        for i in range(4):
            z = co[i, rows, :].astype(F32) + r2o[i, rows, :].astype(F32)
            hb[core * 4 + i, rows, :] = (xb[core * 4 + i, rows, :].astype(F32) + z).astype(BF16)
        remote3o(q).start()

    def finish_o(q, l):
        remote3o(q).wait_recv()
        norm_rows(hb, q * QR, g_mlp, l)

    def remote1m(hf, i):
        rows = pl.ds(hf * HR, HR)
        return remote(tm.at[(1 - core) * 4 + i, rows], r1m.at[i, rows], s1m.at[hf, i], a1m.at[hf, i], partner)

    def remote2m(hf, i):
        rows = pl.ds(hf * HR, HR)
        return remote(cm.at[i, rows], r2m.at[i, rows], s2m.at[hf, i], a2m.at[hf, i], across)

    def remote3m(hf, i):
        rows = pl.ds(hf * HR, HR)
        return remote(xb.at[core * 4 + i, rows], xb.at[core * 4 + i, rows], s3m.at[hf, i], a3m.at[hf, i], partner)

    def chip_sum_m(hf, pieces):
        rows = pl.ds(hf * HR, HR)
        for i in pieces:
            remote1m(hf, i).wait_recv()
            cm[i, rows, :] = (tm[core * 4 + i, rows, :].astype(F32) + r1m[i, rows, :].astype(F32)).astype(BF16)
            remote2m(hf, i).start()

    def group_sum_m(hf, pieces):
        rows = pl.ds(hf * HR, HR)
        for i in pieces:
            remote2m(hf, i).wait_recv()
            z = cm[i, rows, :].astype(F32) + r2m[i, rows, :].astype(F32)
            xb[core * 4 + i, rows, :] = (hb[core * 4 + i, rows, :].astype(F32) + z).astype(BF16)
            remote3m(hf, i).start()

    def finish_m(hf):
        for i in range(4):
            remote3m(hf, i).wait_recv()

    def drain_o():
        for q in range(NQ):
            remote1o(q).wait_send()
            remote2o(q).wait_send()
            remote3o(q).wait_send()

    def drain_m(hf):
        for i in range(4):
            remote1m(hf, i).wait_send()
            remote2m(hf, i).wait_send()
            remote3m(hf, i).wait_send()

    def gate_up(l, hf, steps):
        rows = pl.ds(hf * HR, HR)
        for n in steps:
            if hf == 0:
                gcopy(l, n).wait()
                ucopy(l, n).wait()
        for n in steps:
            gate = _dot(an[rows, :], wg[n])
            up = _dot(an[rows, :], wu[n])
            act[rows, n * 512:(n + 1) * 512] = (jax.nn.silu(gate) * up).astype(BF16)

    def down(l, hf):
        rows = pl.ds(hf * HR, HR)
        if hf == 0:
            for i in range(NCB):
                dcopy(l, i).wait()
        for i in range(4):
            theirs, mine = (1 - core) * 4 + i, core * 4 + i
            tm[theirs, rows, :] = _dot(act[rows, :], wd[theirs]).astype(BF16)
            tm[mine, rows, :] = _dot(act[rows, :], wd[mine]).astype(BF16)
            group = 2 if hf == 1 and l + 1 == LAYERS else 4
            if (i + 1) % group == 0:
                for u in range(i + 1 - group, i + 1):
                    remote1m(hf, u).start()

    for i in range(NCB):
        xcopy(i).wait()

    for l in range(LAYERS):
        lead = LEAD[l]
        last = l + 1 == LAYERS

        def when(cond, f):
            if isinstance(cond, bool):
                if cond:
                    f()
            else:
                pl.when(cond)(f)

        def refill_k(c):
            when(c + lead < NCH, lambda: kcopy(l, c + lead).start())

        def refill_v(c):
            when(c + lead < NCH, lambda: vcopy(l, c + lead).start())

        def refill_w(c):
            t = c + lead - NCH

            def gate_and_up():
                for u in range(2):
                    gcopy(l, 2 * t + u).start()
                    ucopy(l, 2 * t + u).start()

            def down_pair():
                for u in range(2):
                    dcopy(l, 2 * (t - 2) + u).start()
                    dcopy(l, 2 * (t - 2) + u + 4).start()
            if isinstance(t, int):
                when(0 <= t < 2, gate_and_up)
                when(2 <= t < 4, down_pair)
            else:
                when(jnp.logical_and(t >= 0, t < 2), gate_and_up)
                when(jnp.logical_and(t >= 2, t < 4), down_pair)

        def piece(k, ahead):
            c = 2 * k
            kcopy(l, c + 1).wait()
            vcopy(l, c).wait()
            vcopy(l, c + 1).wait()
            if ahead:
                kcopy(l, c + 2).wait()
            scores(l, c + 1)
            values(l, c)
            if ahead:
                scores(l, c + 2)
            values(l, c + 1)
            out_proj(k)
            refill_k(c + 1)
            refill_v(c)
            refill_v(c + 1)
            refill_w(c + 1)
            if ahead:
                refill_k(c + 2)
                refill_w(c + 2)

        @pl.loop(0, NQ if l == 0 else NQ // 2)
        def _(q):
            norm_rows(xb, pl.multiple_of(q * QR, QR), g_attn, l)

        for i in range(4):
            qcopy(l, i).wait()
        project(l, 0, ROWS if l == 0 else HR)
        if l == 0:
            pl.semaphore_wait(barrier, 2)
        kcopy(l, 0).wait()
        scores(l, 0)
        refill_k(0)
        refill_w(0)
        for j in range(2):
            ocopy(l, j).wait()
        if l == 0:
            @pl.loop(1, NCH)
            def _(i):
                vcopy(l, i - 1).wait()
                kcopy(l, i).wait()
                scores(l, i)
                values(l, i - 1)
                refill_k(i)
                refill_v(i - 1)
                refill_w(i)

                @pl.when(jnp.logical_and(lax.rem(i, 2) == 0, i >= 2))
                def _():
                    out_proj(i // 2 - 1)

                @pl.when(jnp.logical_and(lax.rem(i, 2) == 1, i >= 3))
                def _():
                    chip_sum_o((i - 3) // 2)

                @pl.when(i == 6)
                def _():
                    group_sum_o(0)

            vcopy(l, NCH - 1).wait()
            values(l, NCH - 1)
            out_proj(3)
        else:
            piece(0, True)
            group_sum_m(1, range(4))
            piece(1, False)
            chip_sum_o(0)
            finish_m(1)
            drain_m(1)

            @pl.loop(NQ // 2, NQ)
            def _(q):
                norm_rows(xb, pl.multiple_of(q * QR, QR), g_attn, l)
            project(l, HR, HR)
            kcopy(l, 4).wait()
            scores(l, 4)
            refill_k(4)
            refill_w(4)
            chip_sum_o(1)
            piece(2, True)
            group_sum_o(0)
            piece(3, False)
            chip_sum_o(2)
        for t in range(max(0, lead), 4):
            for u in range(2):
                dcopy(l, 2 * (t - 2) + u).start()
                dcopy(l, 2 * (t - 2) + u + 4).start()
        if not last:
            for i in range(4):
                qcopy(l + 1, i).start()
        group_sum_o(1)
        finish_o(0, l)
        finish_o(1, l)
        if not last:
            for i in range(2):
                ocopy(l + 1, i).start()
            for c in range(LEAD[l + 1]):
                kcopy(l + 1, c).start()
                vcopy(l + 1, c).start()
        gate_up(l, 0, (0,))
        chip_sum_o(3)
        gate_up(l, 0, (1, 2, 3))
        group_sum_o(2)
        down(l, 0)
        group_sum_o(3)
        chip_sum_m(0, range(4))
        finish_o(2, l)
        finish_o(3, l)
        gate_up(l, 1, range(4))
        down(l, 1)
        drain_o()
        group_sum_m(0, range(4))
        chip_sum_m(1, range(4))
        finish_m(0)
        drain_m(0)
        if last:
            group_sum_m(1, range(4))
            finish_m(1)
            drain_m(1)

    for i in range(NCB):
        out_ref[:, i * CB:(i + 1) * CB] = xb[i]


def solution(mesh):
    half = HD // 2
    freq = np.float32(ROPE_THETA) ** (-np.arange(half, dtype=np.float32) * np.float32(2.0) / np.float32(HD))
    freq = np.tile(freq.astype(np.float32), 4)[None, :]

    def body(x, g_attn, w_qkv, w_o, g_mlp, w_gate, w_up, w_down, k_cache, v_cache, lengths):
        kt = jnp.transpose(k_cache, (0, 1, 3, 4, 2)).reshape(LAYERS, ROWS, 2 * HD, SEQ)
        vt = jnp.transpose(v_cache, (0, 1, 3, 4, 2)).reshape(LAYERS, ROWS * 2 * HD, SEQ)
        vm, hbm, sm = (pl.BlockSpec(memory_space=s) for s in (pltpu.VMEM, pl.ANY, pltpu.SMEM))
        V, DMA = pltpu.VMEM, pltpu.SemaphoreType.DMA
        scratch = [
            V((RING, CHUNK, 2 * HD, SEQ), BF16), V((RING, CHUNK * 2 * HD, SEQ), BF16),
            V((D, QKVL), BF16), V((512, D), BF16), V((4, D, 512), BF16), V((4, D, 512), BF16), V((NCB, FFL, CB), BF16),
            V((NCB, ROWS, CB), BF16), V((NCB, ROWS, CB), BF16), V((ROWS, D), BF16), V((ROWS, FFL), BF16),
            V((NCB, ROWS, CB), BF16), V((NCB, ROWS, CB), BF16),
            V((4, ROWS, CB), BF16), V((4, ROWS, CB), BF16), V((4, ROWS, CB), BF16), V((4, ROWS, CB), BF16),
            V((4, ROWS, CB), BF16), V((4, ROWS, CB), BF16),
            V((6, ROWS, 128), F32), V((ROWS * HEADS, 128), F32), V((256, 128), F32),
            V((ROWS, 128), F32), V((ROWS, 128), F32), V((ROWS, 128), F32), V((ROWS, 128), F32),
            V((2, 128, SEQ), BF16), V((4, 2, 128, 128), F32), V((2, 128, 128), F32),
            DMA((RING,)), DMA((RING,)), DMA((4,)), DMA((2,)), DMA((4,)), DMA((4,)), DMA((NCB,)), DMA((NCB,)),
        ] + [DMA((4,)) for _ in range(6)] + [DMA((2, 4)) for _ in range(6)]
        return pl.pallas_call(
            _kernel,
            out_shape=pltpu.VMEM((ROWS, D), BF16),
            in_specs=[sm, vm, vm, vm, vm] + [hbm] * 8,
            out_specs=vm,
            scratch_shapes=scratch,
            compiler_params=pltpu.CompilerParams(collective_id=0, has_side_effects=True,
                                                 vmem_limit_bytes=VMEM_LIMIT),
            name="decoder",
        )(lengths, lengths.reshape(1, ROWS), jnp.asarray(freq), g_attn, g_mlp, x, w_qkv, w_o, w_gate, w_up, w_down,
          kt, vt)

    col = P(None, None, 'tp')
    row = P(None, 'tp', None)
    cache = P(None, 'dp', None, 'tp', None)
    return jax.shard_map(body, mesh=mesh,
                         in_specs=(P('dp', None), P(), col, row, P(), col, col, row, cache, cache, P('dp')),
                         out_specs=P('dp', None), check_vma=False)
```
